32 devices in a mesh: tm: 8 (over y, x, core), space: 4 (over z).
Axes of the slice: x: 2, y: 2, z: 4, core: 2. Of those that a mesh axis runs over, the one named last changes fastest.
Arguments:
- trajectory: float32 [64, 256, 1024], P('tm', 'space'), may hold values from -1.2 to 1.2
- initial_state: float32 [256, 1024], P('space'), may hold values from -1 to 1
- residual: float32 [64, 256, 1024], P('tm', 'space'), may hold values from -3000 to 3000
- mobility: float32 [256, 1024], P('space'), may hold values from 20 to 200
Outputs:
- update: float32 [64, 256, 1024], P('tm', 'space')
- reduction: float32 [], replicated
The draws below stay inside these ranges and needn't reach their ends.
All inputs are finite; a program needn't handle non-finite values.
Results may differ from the reference program's by a relative error of at most 0.00015.
Values sent between devices are 32-bit elements; how exact they have to be, the bound alone decides.
A program may use at most 64 MiB of HBM per device.

```python
import math
import jax
import jax.numpy as jnp
from jax import lax

NT = 64
NCOL = 1024
SWEEPS = 16
NROWS = 256


def draw_residual(key, part):
    step_pos = jnp.arange(NT).astype(jnp.float32) / (NT - 1)
    row_pos = jnp.arange(NROWS).astype(jnp.float32) / (NROWS - 1)
    envelope = 40.0 * (1.0 + 2.0 * step_pos)[:, None, None] * (1.0 + 2.0 * row_pos)[None, :, None]
    samples = jnp.clip(jax.random.normal(key, (NT, NROWS, NCOL), jnp.float32), -5.0, 5.0)
    return (envelope * samples).astype(jnp.float32)


def block_levels(rng, shape, shards, least, high):
    def one(position, shards_of):
        heights = jax.random.uniform(jax.random.fold_in(jax.random.fold_in(rng, 6), position), (shards_of,), jnp.float32, least / len(shards), high / len(shards))
        return jnp.repeat(jnp.exp(heights), shape[position] // shards_of).reshape((-1,) + (1,) * (len(shape) - position - 1))

    level = one(*shards[0])
    for cut in shards[1:]:
        level = level * one(*cut)
    return level


def setup_inputs(seed: int = 0) -> dict:
    seeds = jax.random.split(jax.random.key(seed), 5)
    return {
        "trajectory": jnp.clip(jax.random.uniform(seeds[0], (NT, NROWS, NCOL), jnp.float32, -1.2, 1.2) * block_levels(seeds[0], (NT, NROWS, NCOL), ((0, 8), (1, 4)), -0.4, 0.0), -1.2, 1.2),
        "initial_state": jnp.clip(jax.random.uniform(seeds[1], (NROWS, NCOL), jnp.float32, -1.0, 1.0) * block_levels(seeds[1], (NROWS, NCOL), ((0, 4),), -0.4, 0.0), -1.0, 1.0),
        "residual": draw_residual(jax.random.fold_in(seeds[4], 71), 0),
        "mobility": jnp.clip(jnp.exp(math.log(200.0) - 2.3025851 * jax.random.uniform(seeds[3], (NROWS, NCOL), jnp.float32) ** block_levels(seeds[3], (NROWS, NCOL), ((0, 4),), -0.2, 0.2)), 20.0, 200.0),
    }


circ_weight = 0.2
time_step = 0.01
damping = 0.8
reaction_scale = 40.0

def time_tables(step_count):
    positions = jnp.arange(step_count).astype(jnp.float32)
    pair_ids = jnp.arange(step_count // 2).astype(jnp.float32)
    phases = 2.0 * jnp.pi * pair_ids / step_count
    angles = phases[:, None] * positions[None, :]
    forward = jnp.stack([jnp.cos(angles), -jnp.sin(angles)], axis=1).reshape(step_count, step_count)
    row_id = jnp.arange(step_count)[:, None]
    forward = jnp.where(row_id == 1, jnp.cos(jnp.pi * positions)[None, :], forward)
    scaling = jnp.where(jnp.arange(step_count) < 2, 1.0, 2.0) / step_count
    inverse = forward.T * scaling[None, :]
    factor = circ_weight ** (1.0 / step_count)
    shift_pair = (1.0 - factor * jnp.cos(phases)) / time_step
    shifts = jnp.stack([shift_pair, shift_pair], axis=1).reshape(step_count)
    shifts = shifts.at[1].set((1.0 + factor) / time_step)
    coupling = factor * jnp.sin(phases) / time_step
    signed = jnp.stack([-coupling, coupling], axis=1).reshape(step_count)
    weights = circ_weight ** (positions / step_count)
    return (forward, inverse, shifts, signed, weights)

def neg_laplace(values):
    neighbours = jnp.roll(values, 1, axis=1) + jnp.roll(values, -1, axis=1)
    neighbours = neighbours + jnp.roll(values, 1, axis=2) + jnp.roll(values, -1, axis=2)
    return 4.0 * values - neighbours

def partner(values):
    extent = values.shape
    return jnp.flip(values.reshape(extent[0] // 2, 2, extent[1], extent[2]), axis=1).reshape(extent)

def relax_pairs(spectrum, shifts, signed, frozen, mobility):
    shift_col = shifts[:, None, None]
    signed_col = signed[:, None, None]
    diagonal = shift_col + (frozen + 4.0 * mobility)[None]
    partner_diag = partner(diagonal)
    denominator = diagonal * partner_diag + signed_col * signed_col

    def one_sweep(sweep_id, values):
        applied = (shift_col + frozen[None]) * values + mobility[None] * neg_laplace(values) + signed_col * partner(values)
        defect = spectrum - applied
        return values + damping * (partner_diag * defect - signed_col * partner(defect)) / denominator
    return lax.fori_loop(0, SWEEPS, one_sweep, jnp.zeros_like(spectrum))

def precondition(values, frozen, mobility, tables):
    forward, inverse, shifts, signed, weights = tables
    weighted = weights[:, None, None] * values
    spectrum = jnp.einsum('mj,jrc->mrc', forward, weighted, precision=lax.Precision.HIGHEST)
    solved = relax_pairs(spectrum, shifts, signed, frozen, mobility)
    restored = jnp.einsum('jm,mrc->jrc', inverse, solved, precision=lax.Precision.HIGHEST)
    return restored / weights[:, None, None]

def jacobian(values, trajectory, mobility):
    earlier = jnp.concatenate([jnp.zeros_like(values[:1]), values[:-1]], axis=0)
    reaction = reaction_scale * (3.0 * trajectory * trajectory - 1.0)
    return (values - earlier) / time_step + mobility[None] * neg_laplace(values) + reaction * values

def reference(trajectory, initial_state, residual, mobility):
    tables = time_tables(NT)
    frozen = reaction_scale * jnp.maximum(3.0 * initial_state * initial_state - 1.0, 0.0)
    norm_value = jnp.sqrt(jnp.sum(residual * residual))
    unit_residual = residual / norm_value
    direction = precondition(unit_residual, frozen, mobility, tables)
    applied = jacobian(direction, trajectory, mobility)
    projection = jnp.sum(unit_residual * applied)
    rest_part = applied - projection * unit_residual
    remainder = jnp.sum(rest_part * rest_part)
    squared_sum = projection * projection + remainder
    update = norm_value * projection / squared_sum * direction
    reduction = jnp.sqrt(remainder / squared_sum)
    return (update, reduction)
```

```python
import functools
import math
import numpy as np
import jax
import jax.numpy as jnp
from jax import lax
from jax.experimental import pallas as pl
from jax.experimental.pallas import tpu as pltpu
from jax.sharding import PartitionSpec as P

SWEEPS = 16
SUB = 8
LANES = 128

circ_weight = 0.2
time_step = 0.01
damping = 0.8
reaction_scale = 40.0

MESH = pl.DeviceIdType.MESH
HIGHEST = lax.Precision.HIGHEST


def time_tables(count):
    f32 = np.float32
    positions = np.arange(count, dtype=f32)
    pair_ids = np.arange(count // 2, dtype=f32)
    phases = f32(2.0 * np.pi) * pair_ids / f32(count)
    angles = phases[:, None] * positions[None, :]
    forward = np.stack([np.cos(angles), -np.sin(angles)], axis=1).reshape(count, count)
    forward[1] = np.cos(f32(np.pi) * positions)
    inverse = forward.T * np.where(np.arange(count) < 2, f32(1.0), f32(2.0)) / f32(count)
    factor = circ_weight ** (1.0 / count)
    shifts = np.repeat((1.0 - factor * np.cos(phases)) / time_step, 2)
    shifts[1] = (1.0 + factor) / time_step
    coupling = factor * np.sin(phases) / time_step
    weights = circ_weight ** (np.arange(count) / count)
    order = np.arange(count).reshape(-1, SUB, 2).transpose(0, 2, 1).reshape(count)
    forward = (forward * weights[None, :])[order]
    inverse = (inverse / weights[:, None])[:, order]
    tiles = np.stack(
        [shifts[0::2].reshape(-1, SUB), shifts[1::2].reshape(-1, SUB), -coupling.reshape(-1, SUB)], axis=1
    )
    tiles = np.broadcast_to(tiles[..., None], tiles.shape + (LANES,))
    return forward.astype(f32), inverse.astype(f32), np.ascontiguousarray(tiles, dtype=f32)


class Plan:
    def __init__(self, t_count, z_count, steps, rows, cols, split):
        self.t, self.z = t_count, z_count
        self.k, self.rows, self.cols = steps, rows, cols
        self.q = split
        self.blocks = t_count // split
        self.r, self.c = rows * split // t_count, cols // split
        outer = 1 << (int(math.log2(t_count)) // 2)
        while self.blocks % outer:
            outer //= 2
        self.inner = self.blocks // outer

    def block_of(self, i, z):
        span = self.q * self.inner
        o, h, n = i // span, (i // self.inner) % self.q, i % self.inner
        b = o * self.inner + n + (o % 2) * (self.inner - 1 - 2 * n)
        return b + (z % 2) * (self.blocks - 1 - 2 * b), h

    def device_of(self, b, h, z):
        b = b + (z % 2) * (self.blocks - 1 - 2 * b)
        o, n = b // self.inner, b % self.inner
        n = n + (o % 2) * (self.inner - 1 - 2 * n)
        return o * self.q * self.inner + h * self.inner + n

    def row_neighbour(self, b, h, z, step):
        total = self.blocks * self.z
        g = (z * self.blocks + b + step + total) % total
        z2, b2 = g // self.blocks, g % self.blocks
        return {"tm": self.device_of(b2, h, z2), "space": z2}


def fold(v):
    total = v[:, :LANES]
    for i in range(1, v.shape[1] // LANES):
        total = total + v[:, i * LANES : (i + 1) * LANES]
    return total


def step_kernel(
    plan, phi_ref, psi_ref, tab_ref, x_ref, traj_ref, base_ref, mob_ref, dir_ref, sums_ref,
    got, y, gain, cross, start, out, prev, z_out, z_got, base_loc, mob_loc, t_got, z_own, zs_got,
    col_out, col_got,
    in_send, in_recv, row_send, row_recv, col_send, col_recv, back_send, back_recv, prev_send, prev_recv,
    edge_send, edge_recv, t_send, t_recv, z_send, z_recv,
):
    K, R, C, Q, T, Z = plan.k, plan.r, plan.c, plan.q, plan.t, plan.z
    NT, CT = K * T, C // LANES
    G = NT // (2 * SUB)
    rows, cols = plan.rows, plan.cols
    keep = 1.0 - damping
    me, z = lax.axis_index("tm"), lax.axis_index("space")
    b, h = plan.block_of(me, z)
    up, down = plan.row_neighbour(b, h, z, -1), plan.row_neighbour(b, h, z, 1)
    left = {"tm": plan.device_of(b, (h + Q - 1) % Q, z)}
    right = {"tm": plan.device_of(b, (h + 1) % Q, z)}
    region = b * Q + h

    barrier = pltpu.get_barrier_semaphore()
    for i in range(1, T):
        pl.semaphore_signal(barrier, inc=1, device_id={"tm": (me + i) % T}, device_id_type=MESH)
    for i in range(1, Z):
        pl.semaphore_signal(barrier, inc=1, device_id={"space": (z + i) % Z}, device_id_type=MESH)
    pl.semaphore_wait(barrier, T + Z - 2)

    def rows_of(blk):
        return pl.ds(pl.multiple_of(blk * R, SUB), R)

    def cols_of(part):
        return pl.ds(pl.multiple_of(part * C, LANES), C)

    def lane_tile(part, j):
        return pl.ds(pl.multiple_of(part * C + j * LANES, LANES), LANES)

    def sent_in(j, i):
        g = (region + i) % T
        gb, gh = g // Q, g % Q
        return pltpu.make_async_remote_copy(
            src_ref=x_ref.at[:, rows_of(gb), lane_tile(gh, j)],
            dst_ref=got.at[j, pl.ds(me * K, K)],
            send_sem=in_send.at[j, i], recv_sem=in_recv.at[j, i],
            device_id={"tm": plan.device_of(gb, gh, z)}, device_id_type=MESH,
        )

    def send_in(j, _):
        for i in range(1, T):
            sent_in(j, i).start()
        return 0

    lax.fori_loop(0, CT, send_in, 0)
    for j in range(CT):
        got[j, pl.ds(me * K, K)] = x_ref[:, rows_of(b), lane_tile(h, j)]
    base_loc[...] = base_ref[rows_of(b), cols_of(h)]
    mob_loc[...] = mob_ref[rows_of(b), cols_of(h)]

    flat = got.reshape(CT, NT * R, LANES)
    WIDE = 2 if CT % 2 == 0 else 1
    CH = WIDE * LANES

    def transform(j, _):
        span = pl.ds(pl.multiple_of(j * CH, LANES), CH)
        for w in range(WIDE):
            for i in range(1, T):
                sent_in(j * WIDE + w, i).wait()
        for r in range(R):
            steps = [flat[j * WIDE + w, pl.ds(r, NT, stride=R), :] for w in range(WIDE)]
            spec = jnp.dot(
                phi_ref[...], jnp.concatenate(steps, axis=1),
                precision=HIGHEST, preferred_element_type=jnp.float32,
            )
            base, mob = base_loc[r : r + 1, span], mob_loc[r : r + 1, span]
            for q in range(G):
                e, o = 2 * SUB * q, 2 * SUB * q + SUB
                s_e, s_o = spec[e : e + SUB], spec[o : o + SUB]
                wide = lambda k: jnp.tile(tab_ref[q, k], (1, CH // LANES))
                d_e, d_o, c = wide(0) + base, wide(1) + base, wide(2)
                scale = damping / (d_e * d_o + c * c)
                b_e = scale * (d_o * s_e - c * s_o)
                b_o = scale * (d_e * s_o + c * s_e)
                scaled = scale * mob
                gain[r, e : e + SUB, span] = scaled * d_o
                gain[r, o : o + SUB, span] = scaled * d_e
                cross[r, q * SUB : (q + 1) * SUB, span] = scaled * c
                start[r, e : e + SUB, span] = b_e
                start[r, o : o + SUB, span] = b_o
                y[0, r + 1, e : e + SUB, span] = b_e
                y[0, r + 1, o : o + SUB, span] = b_o
        return 0

    lax.fori_loop(0, CT // WIDE, transform, 0)

    def tile_of(q):
        return pl.ds(pl.multiple_of(q * 2 * SUB, 2 * SUB), 2 * SUB)

    def row_edge(slot, q, side):
        return pltpu.make_async_remote_copy(
            src_ref=y.at[slot, 1 if side == 0 else R, tile_of(q)],
            dst_ref=y.at[slot, R + 1 if side == 0 else 0, tile_of(q)],
            send_sem=row_send.at[slot, q, side], recv_sem=row_recv.at[slot, q, 1 - side],
            device_id=up if side == 0 else down, device_id_type=MESH,
        )

    def col_edge(slot, q, side):
        return pltpu.make_async_remote_copy(
            src_ref=col_out.at[slot, q, side], dst_ref=col_got.at[slot, q, 1 - side],
            send_sem=col_send.at[slot, q, side], recv_sem=col_recv.at[slot, q, 1 - side],
            device_id=left if side == 0 else right, device_id_type=MESH,
        )

    lane = lax.broadcasted_iota(jnp.int32, (SUB, LANES), 1)

    def packed(total, v, r, side):
        if side == 0:
            v, at = v[:, :LANES], 0
        else:
            v, at = v[:, C - LANES :], LANES - 1
        v = pltpu.roll(v, (r - at) % LANES, 1)
        return jnp.where(lane == r, v, total)

    def start_edges(slot, q):
        for side in range(2):
            row_edge(slot, q, side).start()
            if Q > 1:
                col_edge(slot, q, side).start()

    order = [0, R - 1] + list(range(1, R - 1))

    def first_edges(q, _):
        if Q > 1:
            for part in range(2):
                tile = pl.ds(pl.multiple_of(q * 2 * SUB, SUB) + part * SUB, SUB)
                lo = hi = jnp.zeros((SUB, LANES), jnp.float32)
                for r in range(R):
                    v = y[0, r + 1, tile, :]
                    lo, hi = packed(lo, v, r, 0), packed(hi, v, r, 1)
                col_out[0, q, 0, part] = lo
                col_out[0, q, 1, part] = hi
        start_edges(0, q)
        return 0

    lax.fori_loop(0, G, first_edges, 0)

    def sweep(s, _):
        now = lax.rem(s, 2)
        later = 1 - now

        def one(q, _):
            for side in range(2):
                row_edge(now, q, side).wait()
                if Q > 1:
                    col_edge(now, q, side).wait()
            e_at = pl.multiple_of(q * 2 * SUB, 2 * SUB)
            tiles = (pl.ds(e_at, SUB), pl.ds(e_at + SUB, SUB))
            c_tile = pl.ds(pl.multiple_of(q * SUB, SUB), SUB)
            ends = [[jnp.zeros((SUB, LANES), jnp.float32)] * 2 for _ in range(2)]

            def around(r, part):
                mid = y[now, r + 1, tiles[part], :]
                total = y[now, r, tiles[part], :] + y[now, r + 2, tiles[part], :]
                low, high = pltpu.roll(mid, 1, 1), pltpu.roll(mid, C - 1, 1)
                if Q > 1:
                    shift = lambda side, at: pltpu.roll(col_got[now, q, side, part], (at - r) % LANES, 1)
                    head = jnp.where(lane == 0, shift(0, 0), low[:, :LANES])
                    tail = jnp.where(lane == LANES - 1, shift(1, LANES - 1), high[:, C - LANES :])
                    low = jnp.concatenate([head, low[:, LANES:]], axis=1)
                    high = jnp.concatenate([high[:, : C - LANES], tail], axis=1)
                return mid, total + (low + high)

            for n, r in enumerate(order):
                y_e, n_e = around(r, 0)
                y_o, n_o = around(r, 1)
                c = cross[r, c_tile, :]
                new_e = keep * y_e + start[r, tiles[0], :] + (gain[r, tiles[0], :] * n_e - c * n_o)
                new_o = keep * y_o + start[r, tiles[1], :] + (gain[r, tiles[1], :] * n_o + c * n_e)
                y[later, r + 1, tiles[0], :] = new_e
                y[later, r + 1, tiles[1], :] = new_o
                if Q > 1:
                    for part, new in enumerate((new_e, new_o)):
                        for side in range(2):
                            ends[part][side] = packed(ends[part][side], new, r, side)
                if n == 1:

                    @pl.when(s < SWEEPS - 2)
                    def _():
                        for side in range(2):
                            row_edge(later, q, side).start()

            if Q > 1:
                for part in range(2):
                    for side in range(2):
                        col_out[later, q, side, part] = ends[part][side]

                @pl.when(s < SWEEPS - 2)
                def _():
                    for side in range(2):
                        col_edge(later, q, side).start()

            return 0

        return lax.fori_loop(0, G, one, 0)

    lax.fori_loop(0, SWEEPS - 1, sweep, 0)
    last = (SWEEPS - 1) % 2

    flat_out = out.reshape(CT, NT * R, LANES)

    def sent_back(j, i):
        g = (me + i) % T
        return pltpu.make_async_remote_copy(
            src_ref=out.at[j, pl.ds(g * K, K)], dst_ref=dir_ref.at[:, rows_of(b), lane_tile(h, j)],
            send_sem=back_send.at[j, i], recv_sem=back_recv.at[j, i],
            device_id={"tm": g}, device_id_type=MESH,
        )

    def sent_prev(j, i):
        g = (me + i) % T
        return pltpu.make_async_remote_copy(
            src_ref=out.at[j, (g * K + NT - 1) % NT], dst_ref=prev.at[rows_of(b), lane_tile(h, j)],
            send_sem=prev_send.at[j, i], recv_sem=prev_recv.at[j, i],
            device_id={"tm": g}, device_id_type=MESH,
        )

    def restore(j, _):
        span = pl.ds(pl.multiple_of(j * CH, LANES), CH)
        for r in range(R):
            steps = jnp.dot(
                psi_ref[...], y[last, r + 1, :, span],
                precision=HIGHEST, preferred_element_type=jnp.float32,
            )
            for w in range(WIDE):
                flat_out[j * WIDE + w, pl.ds(r, NT, stride=R), :] = steps[:, w * LANES : (w + 1) * LANES]
        for w in range(WIDE):
            for i in range(1, T):
                sent_back(j * WIDE + w, i).start()
                sent_prev(j * WIDE + w, i).start()
        return 0

    lax.fori_loop(0, CT // WIDE, restore, 0)
    for j in range(CT):
        dir_ref[:, rows_of(b), lane_tile(h, j)] = out[j, pl.ds(me * K, K)]
        prev[rows_of(b), lane_tile(h, j)] = out[j, (me * K + NT - 1) % NT]

    def arrive(j, _):
        for i in range(1, T):
            sent_back(j, i).wait()
            sent_prev(j, i).wait()
        return 0

    lax.fori_loop(0, CT, arrive, 0)

    for k in range(K):
        z_out[0, k : k + 1, :] = dir_ref[k, 0:1, :]
        z_out[1, k : k + 1, :] = dir_ref[k, rows - 1 : rows, :]
    edges = []
    for side in range(2):
        edges.append(
            pltpu.make_async_remote_copy(
                src_ref=z_out.at[side], dst_ref=z_got.at[1 - side],
                send_sem=edge_send.at[side], recv_sem=edge_recv.at[1 - side],
                device_id={"space": (z + (Z - 1 if side == 0 else 1)) % Z}, device_id_type=MESH,
            )
        )
    for copy in edges:
        copy.start()
    sub = lax.broadcasted_iota(jnp.int32, (SUB, cols), 0)
    has_prev = jnp.minimum(me, 1).astype(jnp.float32)
    tiles = rows // SUB

    def tile_sums(k, first, t, acc):
        span = pl.ds(t * SUB, SUB)
        v = dir_ref[k, span, :]
        if t == 0:
            above = jnp.where(sub == 0, z_got[0, pl.ds(k, 1), :], pltpu.roll(v, 1, 0))
        else:
            above = dir_ref[k, pl.ds(t * SUB - 1, SUB), :]
        if t == tiles - 1:
            below = jnp.where(sub == SUB - 1, z_got[1, pl.ds(k, 1), :], pltpu.roll(v, SUB - 1, 0))
        else:
            below = dir_ref[k, pl.ds(t * SUB + 1, SUB), :]
        near = above + below + (pltpu.roll(v, 1, 1) + pltpu.roll(v, cols - 1, 1))
        before = prev[span, :] * has_prev if first else dir_ref[k - 1, span, :]
        u = traj_ref[k, span, :]
        applied = (v - before) * (1.0 / time_step) + mob_ref[span, :] * (4.0 * v - near)
        applied = applied + reaction_scale * (3.0 * u * u - 1.0) * v
        res = x_ref[k, span, :]
        return acc[0] + fold(res * res), acc[1] + fold(res * applied), acc[2] + fold(applied * applied)

    zero = jnp.zeros((SUB, LANES), jnp.float32)
    acc = (zero, zero, zero)

    def some(k, first, which, acc):
        for t in which:
            acc = tile_sums(k, first, t, acc)
        return acc

    inner = list(range(1, tiles - 1))
    acc = some(0, True, inner, acc)
    acc = lax.fori_loop(1, K, lambda k, a: some(k, False, inner, a), acc)
    for copy in edges:
        copy.wait()
    acc = some(0, True, [0, tiles - 1], acc)
    acc = lax.fori_loop(1, K, lambda k, a: some(k, False, [0, tiles - 1], a), acc)

    row = lax.broadcasted_iota(jnp.int32, (SUB, LANES), 0)
    pack = zero
    for n in range(3):
        pack = jnp.where(row == n, jnp.sum(acc[n], axis=0, keepdims=True), pack)
    t_got[me] = pack
    z_own[...] = pack

    def exchange(axis, count, at, src, dst, snd, rcv):
        copies = []
        for i in range(1, count):
            copies.append(
                pltpu.make_async_remote_copy(
                    src_ref=src, dst_ref=dst.at[at], send_sem=snd.at[i], recv_sem=rcv.at[i],
                    device_id={axis: (at + i) % count}, device_id_type=MESH,
                )
            )
        for copy in copies:
            copy.start()
        for copy in copies:
            copy.wait()
        total = dst[0]
        for i in range(1, count):
            total = total + dst[i]
        return total

    part = exchange("tm", T, me, z_own.at[...], t_got, t_send, t_recv)
    z_own[...] = part
    zs_got[z] = part
    sums_ref[...] = exchange("space", Z, z, z_own.at[...], zs_got, z_send, z_recv)


def finish_kernel(sums_ref, dir_ref, out_ref, red_ref):
    sums = jnp.sum(sums_ref[...], axis=1, keepdims=True)
    norm, crossed, squared = sums[0:1], sums[1:2], sums[2:3]
    out_ref[...] = (crossed / squared)[None] * dir_ref[...]
    projection, squared_sum = crossed / norm, squared / norm
    remainder = jnp.maximum(squared_sum - projection * projection, 0.0)
    red_ref[...] = jnp.sqrt(remainder / squared_sum)


def column_split(t_count, rows):
    return max(1, t_count * SUB // rows)


def on_device(trajectory, initial_state, residual, mobility):
    t_count, z_count = lax.axis_size("tm"), lax.axis_size("space")
    steps, rows, cols = residual.shape
    plan = Plan(t_count, z_count, steps, rows, cols, column_split(t_count, rows))
    count = steps * t_count
    groups = count // (2 * SUB)
    forward, inverse, tables = time_tables(count)
    frozen = reaction_scale * jnp.maximum(3.0 * initial_state * initial_state - 1.0, 0.0)
    R, C, tiles = plan.r, plan.c, plan.c // LANES
    f32 = jnp.float32
    vmem = pl.BlockSpec(memory_space=pltpu.VMEM)
    dma = pltpu.SemaphoreType.DMA
    V = lambda *shape: pltpu.VMEM(shape, f32)
    direction, sums = pl.pallas_call(
        functools.partial(step_kernel, plan),
        out_shape=[jax.ShapeDtypeStruct(residual.shape, f32), jax.ShapeDtypeStruct((SUB, LANES), f32)],
        in_specs=[vmem] * 7,
        out_specs=[vmem, vmem],
        scratch_shapes=[
            V(tiles, count, R, LANES), V(2, R + 2, count, C), V(R, count, C), V(R, count // 2, C), V(R, count, C),
            V(tiles, count, R, LANES), V(rows, cols), V(2, steps, cols), V(2, steps, cols), V(R, C), V(R, C),
            V(t_count, SUB, LANES), V(SUB, LANES), V(z_count, SUB, LANES),
            V(2, groups, 2, 2, SUB, LANES), V(2, groups, 2, 2, SUB, LANES),
            dma((tiles, t_count)), dma((tiles, t_count)), dma((2, groups, 2)), dma((2, groups, 2)),
            dma((2, groups, 2)), dma((2, groups, 2)), dma((tiles, t_count)), dma((tiles, t_count)),
            dma((tiles, t_count)), dma((tiles, t_count)), dma((2,)), dma((2,)),
            dma((t_count,)), dma((t_count,)), dma((z_count,)), dma((z_count,)),
        ],
        compiler_params=pltpu.CompilerParams(
            collective_id=0, has_side_effects=True, vmem_limit_bytes=48 * 1024 * 1024
        ),
    )(jnp.asarray(forward), jnp.asarray(inverse), jnp.asarray(tables), residual, trajectory, frozen + 4.0 * mobility, mobility)
    update, reduction = pl.pallas_call(
        finish_kernel,
        grid=(steps,),
        out_shape=[jax.ShapeDtypeStruct(residual.shape, f32), jax.ShapeDtypeStruct((1, 1), f32)],
        in_specs=[
            pl.BlockSpec((SUB, LANES), lambda i: (0, 0)),
            pl.BlockSpec((1, rows, cols), lambda i: (i, 0, 0)),
        ],
        out_specs=[
            pl.BlockSpec((1, rows, cols), lambda i: (i, 0, 0)),
            pl.BlockSpec((1, 1), lambda i: (0, 0)),
        ],
    )(sums, direction)
    return (update, reduction[0, 0])


def solution(mesh):
    placed = (P("tm", "space", None), P("space", None), P("tm", "space", None), P("space", None))
    return jax.shard_map(
        on_device,
        mesh=mesh,
        in_specs=placed,
        out_specs=(P("tm", "space", None), P()),
        check_vma=False,
    )
```

```python
import functools
import math
import numpy as np
import jax
import jax.numpy as jnp
from jax import lax
from jax.experimental import pallas as pl
from jax.experimental.pallas import tpu as pltpu
from jax.sharding import PartitionSpec as P

SWEEPS = 16
DEPTH = 3
SUB = 8
LANES = 128

circ_weight = 0.2
time_step = 0.01
damping = 0.8
reaction_scale = 40.0

MESH = pl.DeviceIdType.MESH
HIGHEST = lax.Precision.HIGHEST


def time_tables(count):
    f32 = np.float32
    positions = np.arange(count, dtype=f32)
    pair_ids = np.arange(count // 2, dtype=f32)
    phases = f32(2.0 * np.pi) * pair_ids / f32(count)
    angles = phases[:, None] * positions[None, :]
    forward = np.stack([np.cos(angles), -np.sin(angles)], axis=1).reshape(count, count)
    forward[1] = np.cos(f32(np.pi) * positions)
    inverse = forward.T * np.where(np.arange(count) < 2, f32(1.0), f32(2.0)) / f32(count)
    factor = circ_weight ** (1.0 / count)
    shifts = np.repeat((1.0 - factor * np.cos(phases)) / time_step, 2)
    shifts[1] = (1.0 + factor) / time_step
    coupling = factor * np.sin(phases) / time_step
    weights = circ_weight ** (np.arange(count) / count)
    order = np.arange(count).reshape(-1, SUB, 2).transpose(0, 2, 1).reshape(count)
    forward = (forward * weights[None, :])[order]
    inverse = (inverse / weights[:, None])[:, order]
    tiles = np.stack(
        [shifts[0::2].reshape(-1, SUB), shifts[1::2].reshape(-1, SUB), -coupling.reshape(-1, SUB)], axis=1
    )
    tiles = np.broadcast_to(tiles[..., None], tiles.shape + (LANES,))
    return forward.astype(f32), inverse.astype(f32), np.ascontiguousarray(tiles, dtype=f32)


class Plan:
    def __init__(self, t_count, z_count, steps, rows, cols):
        self.t, self.z = t_count, z_count
        self.k, self.rows, self.cols = steps, rows, cols
        self.r = rows // t_count
        self.tiles = cols // LANES
        self.ring = t_count // 2

    def strip_of(self, i, z):
        chip, core = i // 2, i % 2
        half = self.ring // 2
        place = chip + (chip // half) * (self.ring + half - 1 - 2 * chip)
        return ((place + z) % self.ring) * 2 + core

    def device_of(self, strip, z):
        place, core = (strip // 2 + self.ring - z % self.ring) % self.ring, strip % 2
        half = self.ring // 2
        chip = place + (place // half) * (self.ring + half - 1 - 2 * place)
        return chip * 2 + core

    def neighbour(self, strip, z, step):
        total = self.t * self.z
        g = (z * self.t + strip + step + total) % total
        z2, s2 = g // self.t, g % self.t
        return {"tm": self.device_of(s2, z2), "space": z2}


def permuted(tiles):
    lane = lax.broadcasted_iota(jnp.int32, tiles[0].shape, 1)
    tiles, bit = list(tiles), 1
    while bit < len(tiles):
        high = (lane // bit) % 2 == 1
        for i in range(len(tiles)):
            if not i & bit:
                a, b = tiles[i], tiles[i + bit]
                tiles[i] = jnp.where(high, pltpu.roll(b, bit, 1), a)
                tiles[i + bit] = jnp.where(high, b, pltpu.roll(a, LANES - bit, 1))
        bit *= 2
    return tiles


def from_left(v, count):
    lane = lax.broadcasted_iota(jnp.int32, v.shape, 1)
    low = jnp.where(lane == 0, pltpu.roll(v, 1, 1), pltpu.roll(v, (count + 1) % LANES, 1))
    return jnp.where(lane < count, low, pltpu.roll(v, count % LANES, 1))


def from_right(v, count):
    lane = lax.broadcasted_iota(jnp.int32, v.shape, 1)
    high = jnp.where(lane == LANES - 1, pltpu.roll(v, LANES - 1, 1), pltpu.roll(v, LANES - 1 - count, 1))
    return jnp.where(lane >= LANES - count, high, pltpu.roll(v, LANES - count, 1))


def fold(v):
    total = v[:, :LANES]
    for i in range(1, v.shape[1] // LANES):
        total = total + v[:, i * LANES : (i + 1) * LANES]
    return total


def step_kernel(
    plan, phi_ref, psi_ref, tab_ref, x_hbm, traj_hbm, init_hbm, mob_hbm, dir_ref, stat_ref,
    x_ref, traj_ref, mob_ref, init_ext, mob_ext, wide_init, wide_mob, got, state, temp, gain, cross, start, out, prev,
    z_out, z_got, t_got, z_own, zs_got,
    load_sem, ext_send, ext_recv, in_send, in_recv, row_send, row_recv, back_send, back_recv,
    prev_send, prev_recv, edge_send, edge_recv, t_send, t_recv, z_send, z_recv,
):
    K, R, T, Z, CT, H = plan.k, plan.r, plan.t, plan.z, plan.tiles, DEPTH
    rows, cols = plan.rows, plan.cols
    NT = K * T
    G = NT // (2 * SUB)
    keep = 1.0 - damping
    me, z = lax.axis_index("tm"), lax.axis_index("space")
    strip = plan.strip_of(me, z)
    up, down = plan.neighbour(strip, z, -1), plan.neighbour(strip, z, 1)

    barrier = pltpu.get_barrier_semaphore()
    for i in range(1, T):
        pl.semaphore_signal(barrier, inc=1, device_id={"tm": (me + i) % T}, device_id_type=MESH)
    for i in range(1, Z):
        pl.semaphore_signal(barrier, inc=1, device_id={"space": (z + i) % Z}, device_id_type=MESH)
    for other in (up, down):
        pl.semaphore_signal(barrier, inc=1, device_id=other, device_id_type=MESH)

    loads = [
        pltpu.make_async_copy(init_hbm, init_ext.at[pl.ds(1, T)], load_sem.at[0]),
        pltpu.make_async_copy(mob_hbm, mob_ext.at[pl.ds(1, T)], load_sem.at[1]),
        pltpu.make_async_copy(x_hbm, x_ref, load_sem.at[2]),
        pltpu.make_async_copy(mob_hbm, mob_ref, load_sem.at[3]),
        pltpu.make_async_copy(traj_hbm, traj_ref, load_sem.at[4]),
    ]
    for copy in loads:
        copy.start()
    pl.semaphore_wait(barrier, T + Z)

    def lane_tile(j):
        return pl.ds(pl.multiple_of(j * LANES, LANES), LANES)

    def sent_in(j, i):
        other = (strip + i) % T
        return pltpu.make_async_remote_copy(
            src_ref=x_hbm.at[:, other, :, lane_tile(j)],
            dst_ref=got.at[j, pl.ds(me * K, K)],
            send_sem=in_send.at[j, i], recv_sem=in_recv.at[j, i],
            device_id={"tm": plan.device_of(other, z)}, device_id_type=MESH,
        )

    def send_in(j, _):
        for i in range(1, T):
            sent_in(j, i).start()
        return 0

    lax.fori_loop(0, CT, send_in, 0)

    beyond = []
    for n, (src, ext) in enumerate(((init_hbm, init_ext), (mob_hbm, mob_ext))):
        for side in range(2):
            beyond.append(
                pltpu.make_async_remote_copy(
                    src_ref=src.at[0 if side == 0 else T - 1],
                    dst_ref=ext.at[T + 1 if side == 0 else 0],
                    send_sem=ext_send.at[n, side], recv_sem=ext_recv.at[n, 1 - side],
                    device_id={"space": (z + (Z - 1 if side == 0 else 1)) % Z}, device_id_type=MESH,
                )
            )
    for copy in beyond:
        copy.start()

    for copy in loads[:3]:
        copy.wait()
    for j in range(CT):
        got[j, pl.ds(me * K, K)] = x_ref[:, strip, :, j * LANES : (j + 1) * LANES]
    for copy in beyond:
        copy.wait()

    def tile(t):
        return slice(t * LANES, (t + 1) * LANES)

    for i in range(R + 2 * (H - 1)):
        at = R + i - (H - 1)
        for ext, wide in ((init_ext, wide_init), (mob_ext, wide_mob)):
            line = ext[strip + at // R, at % R : at % R + 1, :]
            wide[i] = jnp.broadcast_to(line, (SUB, cols))

    def prepare(i, _):
        mobs, bases = [], []
        for t in range(CT):
            u, m = wide_init[i, :, tile(t)], wide_mob[i, :, tile(t)]
            mobs.append(m)
            bases.append(reaction_scale * jnp.maximum(3.0 * u * u - 1.0, 0.0) + 4.0 * m)
        mobs, bases = permuted(mobs), permuted(bases)
        for q in range(G):
            e, o = pl.ds(2 * SUB * q, SUB), pl.ds(2 * SUB * q + SUB, SUB)
            for t in range(CT):
                d_e, d_o, c = tab_ref[q, 0] + bases[t], tab_ref[q, 1] + bases[t], tab_ref[q, 2]
                scale = damping / (d_e * d_o + c * c)
                a_e, a_o, a_c = scale * d_o, scale * d_e, scale * c
                start[i, e, tile(t)] = a_e
                start[i, o, tile(t)] = a_o
                temp[i, pl.ds(SUB * q, SUB), tile(t)] = a_c
                gain[i, e, tile(t)] = a_e * mobs[t]
                gain[i, o, tile(t)] = a_o * mobs[t]
                cross[i, pl.ds(SUB * q, SUB), tile(t)] = a_c * mobs[t]
        return 0

    lax.fori_loop(0, R + 2 * (H - 1), prepare, 0)

    WIDE = 2 if CT % 2 == 0 else 1
    CH = WIDE * LANES
    strided = R % SUB == 0

    def wide_span(j):
        return pl.ds(pl.multiple_of(j * CH, LANES), CH)

    def transform(j, _):
        for w in range(WIDE):
            for i in range(1, T):
                sent_in(j * WIDE + w, i).wait()
        for r in range(R):
            if strided:
                flat = got.reshape(CT, NT * R, LANES)
                steps = [flat[j * WIDE + w, pl.ds(r, NT, stride=R), :] for w in range(WIDE)]
            else:
                steps = [got[j * WIDE + w, :, r, :] for w in range(WIDE)]
            state[0, r + H, :, wide_span(j)] = jnp.dot(
                phi_ref[...], jnp.concatenate(steps, axis=1),
                precision=HIGHEST, preferred_element_type=jnp.float32,
            )
        return 0

    lax.fori_loop(0, CT // WIDE, transform, 0)

    def group(q):
        return pl.ds(pl.multiple_of(q * 2 * SUB, 2 * SUB), 2 * SUB)

    def row_edge(slot, q, side):
        return pltpu.make_async_remote_copy(
            src_ref=state.at[slot, pl.ds(H if side == 0 else R, H), group(q)],
            dst_ref=state.at[slot, pl.ds(R + H if side == 0 else 0, H), group(q)],
            send_sem=row_send.at[slot, q, side], recv_sem=row_recv.at[slot, q, 1 - side],
            device_id=up if side == 0 else down, device_id_type=MESH,
        )

    def parts_of(q):
        at = pl.multiple_of(q * 2 * SUB, 2 * SUB)
        return pl.ds(at, SUB), pl.ds(at + SUB, SUB), pl.ds(pl.multiple_of(q * SUB, SUB), SUB)

    def first(q, _):
        e, o, c = parts_of(q)
        for r in range(R):
            s_e = permuted([state[0, r + H, e, tile(t)] for t in range(CT)])
            s_o = permuted([state[0, r + H, o, tile(t)] for t in range(CT)])
            i = r + H - 1
            for t in range(CT):
                a_e, a_o, a_c = start[i, e, tile(t)], start[i, o, tile(t)], temp[i, c, tile(t)]
                b_e = a_e * s_e[t] - a_c * s_o[t]
                b_o = a_o * s_o[t] + a_c * s_e[t]
                start[i, e, tile(t)] = b_e
                start[i, o, tile(t)] = b_o
                state[0, r + H, e, tile(t)] = b_e
                state[0, r + H, o, tile(t)] = b_o
        for side in range(2):
            row_edge(0, q, side).start()
        return 0

    lax.fori_loop(0, G, first, 0)

    rounds = (SWEEPS - 1) // H

    def visits(n, _):
        now = lax.rem(n, 2)
        later = 1 - now

        def visit(q, _):
            e, o, c_at = parts_of(q)
            for side in range(2):
                row_edge(now, q, side).wait()

            @pl.when(n == 0)
            def _():
                for r in list(range(1 - H, 0)) + list(range(R, R + H - 1)):
                    start[r + H - 1, group(q), :] = state[0, r + H, group(q), :]

            def from_state(slot):
                return lambda r, part, t: state[slot, r + H, part, tile(t)]

            def from_temp(r, part, t):
                return temp[r + H - 1, part, tile(t)]

            for i in range(1, H + 1):
                source = from_temp if i % 2 == 0 else from_state(now)
                into_temp = i % 2 == 1 and i < H
                slot = later if i == H else now
                for r in range(i - H, R + H - i):
                    y_e = [source(r, e, t) for t in range(CT)]
                    y_o = [source(r, o, t) for t in range(CT)]
                    ends = [(from_left(y[CT - 1], CT), from_right(y[0], CT)) for y in (y_e, y_o)]
                    at = r + H - 1
                    for t in range(CT):

                        def near(y, end, part):
                            low = y[t - 1] if t else end[0]
                            high = y[t + 1] if t < CT - 1 else end[1]
                            return (source(r - 1, part, t) + source(r + 1, part, t)) + (low + high)

                        n_e, n_o = near(y_e, ends[0], e), near(y_o, ends[1], o)
                        c = cross[at, c_at, tile(t)]
                        new_e = keep * y_e[t] + start[at, e, tile(t)] + (gain[at, e, tile(t)] * n_e - c * n_o)
                        new_o = keep * y_o[t] + start[at, o, tile(t)] + (gain[at, o, tile(t)] * n_o + c * n_e)
                        if into_temp:
                            temp[at, e, tile(t)] = new_e
                            temp[at, o, tile(t)] = new_o
                        else:
                            state[slot, r + H, e, tile(t)] = new_e
                            state[slot, r + H, o, tile(t)] = new_o

            @pl.when(n < rounds - 1)
            def _():
                for side in range(2):
                    row_edge(later, q, side).start()

            return 0

        return lax.fori_loop(0, G, visit, 0)

    lax.fori_loop(0, rounds, visits, 0)
    last = rounds % 2

    def unpermute(m, _):
        part = pl.ds(pl.multiple_of(m * SUB, SUB), SUB)
        for r in range(R):
            for t, v in enumerate(permuted([state[last, r + H, part, tile(t)] for t in range(CT)])):
                temp[r, part, tile(t)] = v
        return 0

    lax.fori_loop(0, NT // SUB, unpermute, 0)

    def sent_back(j, i):
        g = (me + i) % T
        return pltpu.make_async_remote_copy(
            src_ref=out.at[j, pl.ds(g * K, K)], dst_ref=dir_ref.at[:, strip, :, lane_tile(j)],
            send_sem=back_send.at[j, i], recv_sem=back_recv.at[j, i],
            device_id={"tm": g}, device_id_type=MESH,
        )

    def sent_prev(j, i):
        g = (me + i) % T
        return pltpu.make_async_remote_copy(
            src_ref=out.at[j, (g * K + NT - 1) % NT], dst_ref=prev.at[strip, :, lane_tile(j)],
            send_sem=prev_send.at[j, i], recv_sem=prev_recv.at[j, i],
            device_id={"tm": g}, device_id_type=MESH,
        )

    def restore(j, _):
        for r in range(R):
            steps = jnp.dot(
                psi_ref[...], temp[r, :, wide_span(j)],
                precision=HIGHEST, preferred_element_type=jnp.float32,
            )
            for w in range(WIDE):
                if strided:
                    flat = out.reshape(CT, NT * R, LANES)
                    flat[j * WIDE + w, pl.ds(r, NT, stride=R), :] = steps[:, tile(w)]
                else:
                    out[j * WIDE + w, :, r, :] = steps[:, tile(w)]
        for w in range(WIDE):
            for i in range(1, T):
                sent_back(j * WIDE + w, i).start()
                sent_prev(j * WIDE + w, i).start()
        return 0

    lax.fori_loop(0, CT // WIDE, restore, 0)
    for j in range(CT):
        dir_ref[:, strip, :, tile(j)] = out[j, pl.ds(me * K, K)]
        prev[strip, :, tile(j)] = out[j, (me * K + NT - 1) % NT]

    def arrive(j, _):
        for i in range(1, T):
            sent_back(j, i).wait()
            sent_prev(j, i).wait()
        return 0

    lax.fori_loop(0, CT, arrive, 0)
    for copy in loads[3:]:
        copy.wait()

    for k in range(K):
        z_out[0, k : k + 1, :] = dir_ref[k, 0, 0:1, :]
        z_out[1, k : k + 1, :] = dir_ref[k, T - 1, R - 1 : R, :]
    edges = []
    for side in range(2):
        edges.append(
            pltpu.make_async_remote_copy(
                src_ref=z_out.at[side], dst_ref=z_got.at[1 - side],
                send_sem=edge_send.at[side], recv_sem=edge_recv.at[1 - side],
                device_id={"space": (z + (Z - 1 if side == 0 else 1)) % Z}, device_id_type=MESH,
            )
        )
    for copy in edges:
        copy.start()
    sub = lax.broadcasted_iota(jnp.int32, (R, cols), 0)
    has_prev = jnp.minimum(me, 1).astype(jnp.float32)

    def shifted(v, row, side):
        if R == SUB:
            at, by = (0, 1) if side == 0 else (R - 1, R - 1)
            return jnp.where(sub == at, row, pltpu.roll(v, by, 0))
        return jnp.concatenate([row, v[: R - 1]] if side == 0 else [v[1:], row], axis=0)

    def tile_sums(k, is_first, t, acc):
        v = dir_ref[k, t]
        above = z_got[0, pl.ds(k, 1), :] if t == 0 else dir_ref[k, t - 1, R - 1 : R, :]
        below = z_got[1, pl.ds(k, 1), :] if t == T - 1 else dir_ref[k, t + 1, 0:1, :]
        near = shifted(v, above, 0) + shifted(v, below, 1) + (pltpu.roll(v, 1, 1) + pltpu.roll(v, cols - 1, 1))
        before = prev[t] * has_prev if is_first else dir_ref[k - 1, t]
        u = traj_ref[k, t]
        applied = (v - before) * (1.0 / time_step) + mob_ref[t] * (4.0 * v - near)
        applied = applied + reaction_scale * (3.0 * u * u - 1.0) * v
        res = x_ref[k, t]
        return acc[0] + fold(res * res), acc[1] + fold(res * applied), acc[2] + fold(applied * applied)

    zero = jnp.zeros((R, LANES), jnp.float32)
    acc = (zero, zero, zero)

    def some(k, is_first, which, acc):
        for t in which:
            acc = tile_sums(k, is_first, t, acc)
        return acc

    inner = list(range(1, T - 1))
    acc = some(0, True, inner, acc)
    acc = lax.fori_loop(1, K, lambda k, a: some(k, False, inner, a), acc)
    for copy in edges:
        copy.wait()
    acc = some(0, True, [0, T - 1], acc)
    acc = lax.fori_loop(1, K, lambda k, a: some(k, False, [0, T - 1], a), acc)

    row = lax.broadcasted_iota(jnp.int32, (SUB, LANES), 0)
    pack = jnp.zeros((SUB, LANES), jnp.float32)
    for n in range(3):
        pack = jnp.where(row == n, jnp.sum(acc[n], axis=0, keepdims=True), pack)
    t_got[me] = pack
    z_own[...] = pack

    def exchange(axis, count, at, dst, snd, rcv):
        copies = []
        for i in range(1, count):
            copies.append(
                pltpu.make_async_remote_copy(
                    src_ref=z_own, dst_ref=dst.at[at], send_sem=snd.at[i], recv_sem=rcv.at[i],
                    device_id={axis: (at + i) % count}, device_id_type=MESH,
                )
            )
        for copy in copies:
            copy.start()
        for copy in copies:
            copy.wait()
        total = dst[0]
        for i in range(1, count):
            total = total + dst[i]
        return total

    part = exchange("tm", T, me, t_got, t_send, t_recv)
    z_own[...] = part
    zs_got[z] = part
    total = exchange("space", Z, z, zs_got, z_send, z_recv)
    total = jnp.broadcast_to(jnp.sum(total, axis=1, keepdims=True), (SUB, LANES))
    norm, crossed, squared = total[0:1], total[1:2], total[2:3]
    projection, squared_sum = crossed / norm, squared / norm
    remainder = jnp.maximum(squared_sum - projection * projection, 0.0)
    stat_ref[0:1, :] = crossed / squared
    stat_ref[1:2, :] = jnp.sqrt(remainder / squared_sum)


def on_device(trajectory, initial_state, residual, mobility):
    t_count, z_count = lax.axis_size("tm"), lax.axis_size("space")
    steps, rows, cols = residual.shape
    plan = Plan(t_count, z_count, steps, rows, cols)
    count = steps * t_count
    groups = count // (2 * SUB)
    forward, inverse, tables = time_tables(count)
    R, H, tiles = plan.r, DEPTH, plan.tiles
    assert (SWEEPS - 1) % H == 0 and R >= H
    f32 = jnp.float32
    vmem, anywhere = pl.BlockSpec(memory_space=pltpu.VMEM), pl.BlockSpec(memory_space=pl.ANY)
    dma = pltpu.SemaphoreType.DMA
    V = lambda *shape: pltpu.VMEM(shape, f32)
    strips = (steps, t_count, R, cols)
    near = R + 2 * (H - 1)
    direction, stats = pl.pallas_call(
        functools.partial(step_kernel, plan),
        out_shape=[jax.ShapeDtypeStruct(strips, f32), jax.ShapeDtypeStruct((2, LANES), f32)],
        in_specs=[vmem] * 3 + [anywhere] * 4,
        out_specs=[vmem, vmem],
        scratch_shapes=[
            V(*strips), V(*strips), V(t_count, R, cols), V(t_count + 2, R, cols), V(t_count + 2, R, cols),
            V(near, SUB, cols), V(near, SUB, cols),
            V(tiles, count, R, LANES), V(2, R + 2 * H, count, cols), V(near, count, cols),
            V(near, count, cols), V(near, count // 2, cols), V(near, count, cols),
            V(tiles, count, R, LANES), V(t_count, R, cols), V(2, steps, cols), V(2, steps, cols),
            V(t_count, SUB, LANES), V(SUB, LANES), V(z_count, SUB, LANES),
            dma((5,)), dma((2, 2)), dma((2, 2)), dma((tiles, t_count)), dma((tiles, t_count)),
            dma((2, groups, 2)), dma((2, groups, 2)), dma((tiles, t_count)), dma((tiles, t_count)),
            dma((tiles, t_count)), dma((tiles, t_count)), dma((2,)), dma((2,)),
            dma((t_count,)), dma((t_count,)), dma((z_count,)), dma((z_count,)),
        ],
        compiler_params=pltpu.CompilerParams(
            collective_id=0, has_side_effects=True, vmem_limit_bytes=63 * 1024 * 1024
        ),
    )(
        jnp.asarray(forward), jnp.asarray(inverse), jnp.asarray(tables),
        residual.reshape(strips), trajectory.reshape(strips),
        initial_state.reshape(strips[1:]), mobility.reshape(strips[1:]),
    )
    update = stats[0:1, 0:1][None] * direction.reshape(residual.shape)
    return (update, stats[1, 0])


def solution(mesh):
    placed = (P("tm", "space", None), P("space", None), P("tm", "space", None), P("space", None))
    return jax.shard_map(
        on_device,
        mesh=mesh,
        in_specs=placed,
        out_specs=(P("tm", "space", None), P()),
        check_vma=False,
    )
```

```python
import functools
import math
import numpy as np
import jax
import jax.numpy as jnp
from jax import lax
from jax.experimental import pallas as pl
from jax.experimental.pallas import tpu as pltpu
from jax.sharding import PartitionSpec as P

SWEEPS = 16
DEPTH = 3
SUB = 8
LANES = 128

circ_weight = 0.2
time_step = 0.01
damping = 0.8
reaction_scale = 40.0

MESH = pl.DeviceIdType.MESH
HIGHEST = lax.Precision.HIGHEST


def time_tables(count):
    f32 = np.float32
    positions = np.arange(count, dtype=f32)
    pair_ids = np.arange(count // 2, dtype=f32)
    phases = f32(2.0 * np.pi) * pair_ids / f32(count)
    angles = phases[:, None] * positions[None, :]
    forward = np.stack([np.cos(angles), -np.sin(angles)], axis=1).reshape(count, count)
    forward[1] = np.cos(f32(np.pi) * positions)
    inverse = forward.T * np.where(np.arange(count) < 2, f32(1.0), f32(2.0)) / f32(count)
    factor = circ_weight ** (1.0 / count)
    shifts = np.repeat((1.0 - factor * np.cos(phases)) / time_step, 2)
    shifts[1] = (1.0 + factor) / time_step
    coupling = factor * np.sin(phases) / time_step
    weights = circ_weight ** (np.arange(count) / count)
    order = np.arange(count).reshape(-1, SUB, 2).transpose(0, 2, 1).reshape(count)
    forward = (forward * weights[None, :])[order]
    inverse = (inverse / weights[:, None])[:, order]
    tiles = np.stack(
        [shifts[0::2].reshape(-1, SUB), shifts[1::2].reshape(-1, SUB), -coupling.reshape(-1, SUB)], axis=1
    )
    tiles = np.broadcast_to(tiles[..., None], tiles.shape + (LANES,))
    return forward.astype(f32), inverse.astype(f32), np.ascontiguousarray(tiles, dtype=f32)


class Plan:
    def __init__(self, t_count, z_count, steps, rows, cols):
        self.t, self.z = t_count, z_count
        self.k, self.rows, self.cols = steps, rows, cols
        self.r = rows // t_count
        self.tiles = cols // LANES
        self.ring = t_count // 2

    def strip_of(self, i, z):
        chip, core = i // 2, i % 2
        half = self.ring // 2
        place = chip + (chip // half) * (self.ring + half - 1 - 2 * chip)
        return ((place + z) % self.ring) * 2 + core

    def device_of(self, strip, z):
        place, core = (strip // 2 + self.ring - z % self.ring) % self.ring, strip % 2
        half = self.ring // 2
        chip = place + (place // half) * (self.ring + half - 1 - 2 * place)
        return chip * 2 + core

    def neighbour(self, strip, z, step):
        total = self.t * self.z
        g = (z * self.t + strip + step + total) % total
        z2, s2 = g // self.t, g % self.t
        return {"tm": self.device_of(s2, z2), "space": z2}


def permuted(tiles):
    lane = lax.broadcasted_iota(jnp.int32, tiles[0].shape, 1)
    tiles, bit = list(tiles), 1
    while bit < len(tiles):
        high = (lane // bit) % 2 == 1
        for i in range(len(tiles)):
            if not i & bit:
                a, b = tiles[i], tiles[i + bit]
                tiles[i] = jnp.where(high, pltpu.roll(b, bit, 1), a)
                tiles[i + bit] = jnp.where(high, b, pltpu.roll(a, LANES - bit, 1))
        bit *= 2
    return tiles


def from_left(v, count):
    lane = lax.broadcasted_iota(jnp.int32, v.shape, 1)
    low = jnp.where(lane == 0, pltpu.roll(v, 1, 1), pltpu.roll(v, (count + 1) % LANES, 1))
    return jnp.where(lane < count, low, pltpu.roll(v, count % LANES, 1))


def from_right(v, count):
    lane = lax.broadcasted_iota(jnp.int32, v.shape, 1)
    high = jnp.where(lane == LANES - 1, pltpu.roll(v, LANES - 1, 1), pltpu.roll(v, LANES - 1 - count, 1))
    return jnp.where(lane >= LANES - count, high, pltpu.roll(v, LANES - count, 1))


def fold(v):
    total = v[:, :LANES]
    for i in range(1, v.shape[1] // LANES):
        total = total + v[:, i * LANES : (i + 1) * LANES]
    return total


def step_kernel(
    plan, phi_hbm, psi_hbm, tab_hbm, x_hbm, traj_hbm, init_hbm, mob_hbm, dir_ref, stat_ref,
    phi_ref, psi_ref, tab_ref, acc, x_ref, traj_ref, mob_ref, init_ext, mob_ext, wide_init, wide_mob, got, state, temp, gain, cross, start, out, prev,
    z_out, z_got, own_sums, all_sums,
    load_sem, ext_send, ext_recv, in_send, in_recv, row_send, row_recv, back_send, back_recv,
    prev_send, prev_recv, hand_send, hand_recv, edge_send, edge_recv, sum_send, sum_recv, column_in,
):
    K, R, T, Z, CT, H = plan.k, plan.r, plan.t, plan.z, plan.tiles, DEPTH
    rows, cols = plan.rows, plan.cols
    NT = K * T
    G = NT // (2 * SUB)
    keep = 1.0 - damping
    me, z = lax.axis_index("tm"), lax.axis_index("space")
    strip = plan.strip_of(me, z)
    up, down = plan.neighbour(strip, z, -1), plan.neighbour(strip, z, 1)

    barrier = pltpu.get_barrier_semaphore()
    for i in range(1, T):
        pl.semaphore_signal(barrier, inc=1, device_id={"tm": (me + i) % T}, device_id_type=MESH)
    for i in range(1, Z):
        pl.semaphore_signal(barrier, inc=1, device_id={"space": (z + i) % Z}, device_id_type=MESH)
    for other in (up, down):
        pl.semaphore_signal(barrier, inc=1, device_id=other, device_id_type=MESH)

    loads = [
        pltpu.make_async_copy(init_hbm, init_ext.at[pl.ds(1, T)], load_sem.at[0]),
        pltpu.make_async_copy(mob_hbm, mob_ext.at[pl.ds(1, T)], load_sem.at[1]),
        pltpu.make_async_copy(x_hbm, x_ref, load_sem.at[2]),
        pltpu.make_async_copy(tab_hbm, tab_ref, load_sem.at[5]),
        pltpu.make_async_copy(phi_hbm, phi_ref, load_sem.at[6]),
        pltpu.make_async_copy(psi_hbm, psi_ref, load_sem.at[7]),
        pltpu.make_async_copy(mob_hbm, mob_ref, load_sem.at[3]),
        pltpu.make_async_copy(traj_hbm, traj_ref, load_sem.at[4]),
    ]
    for copy in loads:
        copy.start()
    pl.semaphore_wait(barrier, T + Z)
    for i in range(1, T):
        pl.semaphore_signal(column_in, inc=1, device_id={"tm": (me + i) % T}, device_id_type=MESH)

    def lane_tile(j):
        return pl.ds(pl.multiple_of(j * LANES, LANES), LANES)

    def sent_in(j, i):
        other = (strip + i) % T
        return pltpu.make_async_remote_copy(
            src_ref=x_hbm.at[:, other, :, lane_tile(j)],
            dst_ref=got.at[j, pl.ds(me * K, K)],
            send_sem=in_send.at[j, i], recv_sem=in_recv.at[j, i],
            device_id={"tm": plan.device_of(other, z)}, device_id_type=MESH,
        )

    def send_in(j, _):
        for i in range(1, T):
            sent_in(j, i).start()
        return 0

    lax.fori_loop(0, CT, send_in, 0)

    beyond = []
    for n, (src, ext) in enumerate(((init_hbm, init_ext), (mob_hbm, mob_ext))):
        for side in range(2):
            beyond.append(
                pltpu.make_async_remote_copy(
                    src_ref=src.at[0 if side == 0 else T - 1],
                    dst_ref=ext.at[T + 1 if side == 0 else 0],
                    send_sem=ext_send.at[n, side], recv_sem=ext_recv.at[n, 1 - side],
                    device_id={"space": (z + (Z - 1 if side == 0 else 1)) % Z}, device_id_type=MESH,
                )
            )
    for copy in beyond:
        copy.start()

    for copy in loads[:6]:
        copy.wait()
    for j in range(CT):
        got[j, pl.ds(me * K, K)] = x_ref[:, strip, :, j * LANES : (j + 1) * LANES]
    for copy in beyond:
        copy.wait()

    def tile(t):
        return slice(t * LANES, (t + 1) * LANES)

    for i in range(R + 2 * (H - 1)):
        at = R + i - (H - 1)
        for ext, wide in ((init_ext, wide_init), (mob_ext, wide_mob)):
            line = ext[strip + at // R, at % R : at % R + 1, :]
            wide[i] = jnp.broadcast_to(line, (SUB, cols))

    def prepare(i, _):
        mobs, bases = [], []
        for t in range(CT):
            u, m = wide_init[i, :, tile(t)], wide_mob[i, :, tile(t)]
            mobs.append(m)
            bases.append(reaction_scale * jnp.maximum(3.0 * u * u - 1.0, 0.0) + 4.0 * m)
        mobs, bases = permuted(mobs), permuted(bases)
        for q in range(G):
            e, o = pl.ds(2 * SUB * q, SUB), pl.ds(2 * SUB * q + SUB, SUB)
            for t in range(CT):
                d_e, d_o, c = tab_ref[q, 0] + bases[t], tab_ref[q, 1] + bases[t], tab_ref[q, 2]
                scale = damping / (d_e * d_o + c * c)
                a_e, a_o, a_c = scale * d_o, scale * d_e, scale * c
                start[i, e, tile(t)] = a_e
                start[i, o, tile(t)] = a_o
                temp[i, pl.ds(SUB * q, SUB), tile(t)] = a_c
                gain[i, e, tile(t)] = a_e * mobs[t]
                gain[i, o, tile(t)] = a_o * mobs[t]
                cross[i, pl.ds(SUB * q, SUB), tile(t)] = a_c * mobs[t]
        return 0

    lax.fori_loop(0, R + 2 * (H - 1), prepare, 0)

    WIDE = 2 if CT % 2 == 0 else 1
    CH = WIDE * LANES
    strided = R % SUB == 0

    def wide_span(j):
        return pl.ds(pl.multiple_of(j * CH, LANES), CH)

    def transform(j, _):
        for w in range(WIDE):
            for i in range(1, T):
                sent_in(j * WIDE + w, i).wait()
        for r in range(R):
            if strided:
                flat = got.reshape(CT, NT * R, LANES)
                steps = [flat[j * WIDE + w, pl.ds(r, NT, stride=R), :] for w in range(WIDE)]
            else:
                steps = [got[j * WIDE + w, :, r, :] for w in range(WIDE)]
            state[0, r + H, :, wide_span(j)] = jnp.dot(
                phi_ref[...], jnp.concatenate(steps, axis=1),
                precision=HIGHEST, preferred_element_type=jnp.float32,
            )
        return 0

    lax.fori_loop(0, CT // WIDE, transform, 0)

    def group(q):
        return pl.ds(pl.multiple_of(q * 2 * SUB, 2 * SUB), 2 * SUB)

    def row_edge(slot, q, side):
        return pltpu.make_async_remote_copy(
            src_ref=state.at[slot, pl.ds(H if side == 0 else R, H), group(q)],
            dst_ref=state.at[slot, pl.ds(R + H if side == 0 else 0, H), group(q)],
            send_sem=row_send.at[slot, q, side], recv_sem=row_recv.at[slot, q, 1 - side],
            device_id=up if side == 0 else down, device_id_type=MESH,
        )

    def parts_of(q):
        at = pl.multiple_of(q * 2 * SUB, 2 * SUB)
        return pl.ds(at, SUB), pl.ds(at + SUB, SUB), pl.ds(pl.multiple_of(q * SUB, SUB), SUB)

    def first(q, _):
        e, o, c = parts_of(q)
        for r in range(R):
            s_e = permuted([state[0, r + H, e, tile(t)] for t in range(CT)])
            s_o = permuted([state[0, r + H, o, tile(t)] for t in range(CT)])
            i = r + H - 1
            for t in range(CT):
                a_e, a_o, a_c = start[i, e, tile(t)], start[i, o, tile(t)], temp[i, c, tile(t)]
                b_e = a_e * s_e[t] - a_c * s_o[t]
                b_o = a_o * s_o[t] + a_c * s_e[t]
                start[i, e, tile(t)] = b_e
                start[i, o, tile(t)] = b_o
                state[0, r + H, e, tile(t)] = b_e
                state[0, r + H, o, tile(t)] = b_o
        for side in range(2):
            row_edge(0, q, side).start()
        return 0

    lax.fori_loop(0, G, first, 0)

    rounds = (SWEEPS - 1) // H

    def visits(n, _):
        now = lax.rem(n, 2)
        later = 1 - now

        def visit(q, _):
            e, o, c_at = parts_of(q)
            for side in range(2):
                row_edge(now, q, side).wait()

            @pl.when(n == 0)
            def _():
                for r in list(range(1 - H, 0)) + list(range(R, R + H - 1)):
                    start[r + H - 1, group(q), :] = state[0, r + H, group(q), :]

            def from_state(slot):
                return lambda r, part, t: state[slot, r + H, part, tile(t)]

            def from_temp(r, part, t):
                return temp[r + H - 1, part, tile(t)]

            for i in range(1, H + 1):
                source = from_temp if i % 2 == 0 else from_state(now)
                into_temp = i % 2 == 1 and i < H
                slot = later if i == H else now
                for r in range(i - H, R + H - i):
                    y_e = [source(r, e, t) for t in range(CT)]
                    y_o = [source(r, o, t) for t in range(CT)]
                    ends = [(from_left(y[CT - 1], CT), from_right(y[0], CT)) for y in (y_e, y_o)]
                    at = r + H - 1
                    for t in range(CT):

                        def near(y, end, part):
                            low = y[t - 1] if t else end[0]
                            high = y[t + 1] if t < CT - 1 else end[1]
                            return (source(r - 1, part, t) + source(r + 1, part, t)) + (low + high)

                        n_e, n_o = near(y_e, ends[0], e), near(y_o, ends[1], o)
                        c = cross[at, c_at, tile(t)]
                        new_e = keep * y_e[t] + start[at, e, tile(t)] + (gain[at, e, tile(t)] * n_e - c * n_o)
                        new_o = keep * y_o[t] + start[at, o, tile(t)] + (gain[at, o, tile(t)] * n_o + c * n_e)
                        if into_temp:
                            temp[at, e, tile(t)] = new_e
                            temp[at, o, tile(t)] = new_o
                        else:
                            state[slot, r + H, e, tile(t)] = new_e
                            state[slot, r + H, o, tile(t)] = new_o

            @pl.when(n < rounds - 1)
            def _():
                for side in range(2):
                    row_edge(later, q, side).start()

            return 0

        return lax.fori_loop(0, G, visit, 0)

    lax.fori_loop(0, rounds, visits, 0)
    last = rounds % 2

    def unpermute(m, _):
        part = pl.ds(pl.multiple_of(m * SUB, SUB), SUB)
        for r in range(R):
            for t, v in enumerate(permuted([state[last, r + H, part, tile(t)] for t in range(CT)])):
                temp[r, part, tile(t)] = v
        return 0

    lax.fori_loop(0, NT // SUB, unpermute, 0)

    def sent_back(j, i):
        g = (me + i) % T
        return pltpu.make_async_remote_copy(
            src_ref=out.at[j, pl.ds(g * K, K)], dst_ref=dir_ref.at[:, strip, :, lane_tile(j)],
            send_sem=back_send.at[j, i], recv_sem=back_recv.at[j, i],
            device_id={"tm": g}, device_id_type=MESH,
        )

    def sent_prev(j, i):
        g = (me + i) % T
        return pltpu.make_async_remote_copy(
            src_ref=out.at[j, (g * K + NT - 1) % NT], dst_ref=prev.at[strip, :, lane_tile(j)],
            send_sem=prev_send.at[j, i], recv_sem=prev_recv.at[j, i],
            device_id={"tm": g}, device_id_type=MESH,
        )

    def hand_on(j):
        return pltpu.make_async_remote_copy(
            src_ref=dir_ref.at[K - 1, :, :, lane_tile(j)], dst_ref=prev.at[:, :, lane_tile(j)],
            send_sem=hand_send.at[j], recv_sem=hand_recv.at[j],
            device_id={"tm": me + 1 - 2 * (me % 2)}, device_id_type=MESH,
        )

    def z_edge(j, side, g):
        return pltpu.make_async_remote_copy(
            src_ref=z_out.at[j, side, pl.ds(g * K, K)], dst_ref=z_got.at[j, 1 - side],
            send_sem=edge_send.at[j, side, g], recv_sem=edge_recv.at[j, 1 - side],
            device_id={"tm": g, "space": (z + (Z - 1 if side == 0 else 1)) % Z}, device_id_type=MESH,
        )

    def restore(j, _):
        for r in range(R):
            steps = jnp.dot(
                psi_ref[...], temp[r, :, wide_span(j)],
                precision=HIGHEST, preferred_element_type=jnp.float32,
            )
            for w in range(WIDE):
                if strided:
                    flat = out.reshape(CT, NT * R, LANES)
                    flat[j * WIDE + w, pl.ds(r, NT, stride=R), :] = steps[:, tile(w)]
                else:
                    out[j * WIDE + w, :, r, :] = steps[:, tile(w)]
                for side, edge in ((0, 0), (1, R - 1)):
                    if r == edge:
                        z_out[j * WIDE + w, side] = steps[:, tile(w)]
        for w in range(WIDE):
            for side, edge in ((0, 0), (1, T - 1)):

                @pl.when(strip == edge)
                def _():
                    for g in range(T):
                        z_edge(j * WIDE + w, side, g).start()

            for i in range(1, T):
                sent_back(j * WIDE + w, i).start()

                @pl.when((me + i) % T % 2 == 0)
                def _():
                    sent_prev(j * WIDE + w, i).start()

        return 0

    pl.semaphore_wait(column_in, T - 1)
    lax.fori_loop(0, CT // WIDE, restore, 0)
    even = me % 2 == 0
    for j in range(CT):
        dir_ref[:, strip, :, tile(j)] = out[j, pl.ds(me * K, K)]

    @pl.when(even)
    def _():
        for j in range(CT):
            prev[strip, :, tile(j)] = out[j, (me * K + NT - 1) % NT]

    for copy in loads[6:]:
        copy.wait()
    acc[...] = jnp.zeros_like(acc)

    def arrive(j):
        for i in range(1, T):
            sent_back(j, i).wait()

            @pl.when((me + i) % T % 2 == 0)
            def _():
                sent_prev(j, i).wait_send()

        @pl.when(even)
        def _():
            for i in range(1, T):
                sent_prev(j, i).wait_recv()
            hand_on(j).start()

        for side, edge in ((0, 0), (1, T - 1)):

            @pl.when(strip == edge)
            def _():
                for g in range(T):
                    z_edge(j, side, g).wait_send()

            z_edge(j, side, me).wait_recv()

    def handed(j):
        @pl.when(even)
        def _():
            hand_on(j).wait_send()

        @pl.when(me % 2 == 1)
        def _():
            hand_on(j).wait_recv()

    sub = lax.broadcasted_iota(jnp.int32, (R, LANES), 0)
    lane = lax.broadcasted_iota(jnp.int32, (R, LANES), 1)
    has_prev = jnp.minimum(me, 1).astype(jnp.float32)

    def shifted(v, line, side):
        if R == SUB:
            at, by = (0, 1) if side == 0 else (R - 1, R - 1)
            return jnp.where(sub == at, line, pltpu.roll(v, by, 0))
        return jnp.concatenate([line, v[: R - 1]] if side == 0 else [v[1:], line], axis=0)

    def tile_sums(j, k, is_first, t, sums):
        here, west, east = lane_tile(j), lane_tile((j + CT - 1) % CT), lane_tile((j + 1) % CT)
        v = dir_ref[k, t, :, here]
        above = z_got[j, 0, pl.ds(k, 1), :] if t == 0 else dir_ref[k, t - 1, R - 1 : R, here]
        below = z_got[j, 1, pl.ds(k, 1), :] if t == T - 1 else dir_ref[k, t + 1, 0:1, here]
        low = pltpu.roll(jnp.where(lane == LANES - 1, dir_ref[k, t, :, west], v), 1, 1)
        high = pltpu.roll(jnp.where(lane == 0, dir_ref[k, t, :, east], v), LANES - 1, 1)
        near = (shifted(v, above, 0) + shifted(v, below, 1)) + (low + high)
        before = prev[t, :, here] * has_prev if is_first else dir_ref[k - 1, t, :, here]
        u = traj_ref[k, t, :, here]
        applied = (v - before) * (1.0 / time_step) + mob_ref[t, :, here] * (4.0 * v - near)
        applied = applied + (3.0 * reaction_scale * u * u - reaction_scale) * v
        res = x_ref[k, t, :, here]
        return sums[0] + res * res, sums[1] + res * applied, sums[2] + applied * applied

    def add_sums(j, which):
        def some(k, is_first, sums):
            for t in which:
                sums = tile_sums(j, k, is_first, t, sums)
            return sums

        sums = some(0, True, (acc[0], acc[1], acc[2]))
        sums = lax.fori_loop(1, K, lambda k, a: some(k, False, a), sums)
        for n in range(3):
            acc[n] = sums[n]

    arrive(0)
    arrive(1)

    def follow(j, _):
        arrive(j)
        handed(j - 1)
        add_sums(j - 1, range(T))
        return 0

    lax.fori_loop(2, CT, follow, 0)

    def rest(n, _):
        j = (n + CT - 1) % CT
        handed(j)
        add_sums(j, range(T))
        return 0

    lax.fori_loop(0, 2, rest, 0)

    at = lax.broadcasted_iota(jnp.int32, (1, LANES), 1)
    pack = jnp.zeros((1, LANES), jnp.float32)
    for n in range(3):
        pack = jnp.where(at == n, jnp.sum(acc[n]), pack)
    own_sums[...] = pack
    index, total_count = me * Z + z, T * Z
    all_sums[index] = pack

    def sent_sum(i):
        other = (index + i) % total_count
        return pltpu.make_async_remote_copy(
            src_ref=own_sums, dst_ref=all_sums.at[index],
            send_sem=sum_send.at[i], recv_sem=sum_recv.at[i],
            device_id={"tm": other // Z, "space": other % Z}, device_id_type=MESH,
        )

    def send_sum(i, _):
        sent_sum(i).start()
        return 0

    def wait_sum(i, _):
        sent_sum(i).wait()
        return 0

    lax.fori_loop(1, total_count, send_sum, 0)
    lax.fori_loop(1, total_count, wait_sum, 0)
    total = all_sums[0]
    for i in range(1, total_count):
        total = total + all_sums[i]
    norm, crossed, squared = [
        jnp.broadcast_to(jnp.sum(jnp.where(at == n, total, 0.0), axis=1, keepdims=True), (1, LANES)) for n in range(3)
    ]
    projection, squared_sum = crossed / norm, squared / norm
    remainder = jnp.maximum(squared_sum - projection * projection, 0.0)
    stat_ref[0:1, :] = crossed / squared
    stat_ref[1:2, :] = jnp.sqrt(remainder / squared_sum)


def on_device(trajectory, initial_state, residual, mobility):
    t_count, z_count = lax.axis_size("tm"), lax.axis_size("space")
    steps, rows, cols = residual.shape
    plan = Plan(t_count, z_count, steps, rows, cols)
    count = steps * t_count
    groups = count // (2 * SUB)
    forward, inverse, tables = time_tables(count)
    R, H, tiles = plan.r, DEPTH, plan.tiles
    assert (SWEEPS - 1) % H == 0 and R >= H
    f32 = jnp.float32
    vmem, anywhere = pl.BlockSpec(memory_space=pltpu.VMEM), pl.BlockSpec(memory_space=pl.ANY)
    dma = pltpu.SemaphoreType.DMA
    V = lambda *shape: pltpu.VMEM(shape, f32)
    strips = (steps, t_count, R, cols)
    near = R + 2 * (H - 1)
    operands = (
        jnp.asarray(forward), jnp.asarray(inverse), jnp.asarray(tables),
        residual.reshape(strips), trajectory.reshape(strips),
        initial_state.reshape(strips[1:]), mobility.reshape(strips[1:]),
    )
    direction, stats = pl.pallas_call(
        functools.partial(step_kernel, plan),
        out_shape=[jax.ShapeDtypeStruct(strips, f32), jax.ShapeDtypeStruct((2, LANES), f32)],
        in_specs=[anywhere] * 7,
        out_specs=[vmem, vmem],
        scratch_shapes=[
            V(*forward.shape), V(*inverse.shape), V(*tables.shape), V(3, R, LANES), V(*strips), V(*strips), V(t_count, R, cols), V(t_count + 2, R, cols), V(t_count + 2, R, cols),
            V(near, SUB, cols), V(near, SUB, cols),
            V(tiles, count, R, LANES), V(2, R + 2 * H, count, cols), V(near, count, cols),
            V(near, count, cols), V(near, count // 2, cols), V(near, count, cols),
            V(tiles, count, R, LANES), V(t_count, R, cols), V(tiles, 2, count, LANES), V(tiles, 2, steps, LANES),
            V(1, LANES), V(t_count * z_count, 1, LANES),
            dma((8,)), dma((2, 2)), dma((2, 2)), dma((tiles, t_count)), dma((tiles, t_count)),
            dma((2, groups, 2)), dma((2, groups, 2)), dma((tiles, t_count)), dma((tiles, t_count)),
            dma((tiles, t_count)), dma((tiles, t_count)), dma((tiles,)), dma((tiles,)),
            dma((tiles, 2, t_count)), dma((tiles, 2)),
            dma((t_count * z_count,)), dma((t_count * z_count,)), pltpu.SemaphoreType.REGULAR,
        ],
        compiler_params=pltpu.CompilerParams(
            collective_id=0, has_side_effects=True, vmem_limit_bytes=36 * 1024 * 1024
        ),
    )(*[pltpu.with_memory_space_constraint(v, pltpu.HBM) for v in operands])
    update = stats[0:1, 0:1][None] * direction.reshape(residual.shape)
    return (update, stats[1, 0])


def solution(mesh):
    placed = (P("tm", "space", None), P("space", None), P("tm", "space", None), P("space", None))
    return jax.shard_map(
        on_device,
        mesh=mesh,
        in_specs=placed,
        out_specs=(P("tm", "space", None), P()),
        check_vma=False,
    )
```

```python
import functools
import math
import numpy as np
import jax
import jax.numpy as jnp
from jax import lax
from jax.experimental import pallas as pl
from jax.experimental.pallas import tpu as pltpu
from jax.sharding import PartitionSpec as P

SWEEPS = 16
DEPTH = 3
CHUNKS_IN = [4, 2, 1, 1]
CHUNKS_OUT = [2, 2, 2, 1, 1]
SUB = 8
LANES = 128

circ_weight = 0.2
time_step = 0.01
damping = 0.8
reaction_scale = 40.0

MESH = pl.DeviceIdType.MESH
HIGHEST = lax.Precision.HIGHEST


def time_tables(count):
    f32 = np.float32
    positions = np.arange(count, dtype=f32)
    pair_ids = np.arange(count // 2, dtype=f32)
    phases = f32(2.0 * np.pi) * pair_ids / f32(count)
    angles = phases[:, None] * positions[None, :]
    forward = np.stack([np.cos(angles), -np.sin(angles)], axis=1).reshape(count, count)
    forward[1] = np.cos(f32(np.pi) * positions)
    inverse = forward.T * np.where(np.arange(count) < 2, f32(1.0), f32(2.0)) / f32(count)
    factor = circ_weight ** (1.0 / count)
    shifts = np.repeat((1.0 - factor * np.cos(phases)) / time_step, 2)
    shifts[1] = (1.0 + factor) / time_step
    coupling = factor * np.sin(phases) / time_step
    weights = circ_weight ** (np.arange(count) / count)
    order = np.arange(count).reshape(-1, SUB, 2).transpose(0, 2, 1).reshape(count)
    forward = (forward * weights[None, :])[order]
    inverse = (inverse / weights[:, None])[:, order]
    tiles = np.stack(
        [shifts[0::2].reshape(-1, SUB), shifts[1::2].reshape(-1, SUB), -coupling.reshape(-1, SUB)], axis=1
    )
    tiles = np.broadcast_to(tiles[..., None], tiles.shape + (LANES,))
    return forward.astype(f32), inverse.astype(f32), np.ascontiguousarray(tiles, dtype=f32)


class Plan:
    def __init__(self, t_count, z_count, steps, rows, cols):
        self.t, self.z = t_count, z_count
        self.k, self.rows, self.cols = steps, rows, cols
        self.r = rows // t_count
        self.tiles = cols // LANES
        self.ring = t_count // 2

    def strip_of(self, i, z):
        chip, core = i // 2, i % 2
        half = self.ring // 2
        place = chip + (chip // half) * (self.ring + half - 1 - 2 * chip)
        return ((place + z) % self.ring) * 2 + core

    def device_of(self, strip, z):
        place, core = (strip // 2 + self.ring - z % self.ring) % self.ring, strip % 2
        half = self.ring // 2
        chip = place + (place // half) * (self.ring + half - 1 - 2 * place)
        return chip * 2 + core

    def neighbour(self, strip, z, step):
        total = self.t * self.z
        g = (z * self.t + strip + step + total) % total
        z2, s2 = g // self.t, g % self.t
        return {"tm": self.device_of(s2, z2), "space": z2}


def permuted(tiles):
    lane = lax.broadcasted_iota(jnp.int32, tiles[0].shape, 1)
    tiles, bit = list(tiles), 1
    while bit < len(tiles):
        high = (lane // bit) % 2 == 1
        for i in range(len(tiles)):
            if not i & bit:
                a, b = tiles[i], tiles[i + bit]
                tiles[i] = jnp.where(high, pltpu.roll(b, bit, 1), a)
                tiles[i + bit] = jnp.where(high, b, pltpu.roll(a, LANES - bit, 1))
        bit *= 2
    return tiles


def from_left(v, count):
    lane = lax.broadcasted_iota(jnp.int32, v.shape, 1)
    low = jnp.where(lane == 0, pltpu.roll(v, 1, 1), pltpu.roll(v, (count + 1) % LANES, 1))
    return jnp.where(lane < count, low, pltpu.roll(v, count % LANES, 1))


def from_right(v, count):
    lane = lax.broadcasted_iota(jnp.int32, v.shape, 1)
    high = jnp.where(lane == LANES - 1, pltpu.roll(v, LANES - 1, 1), pltpu.roll(v, LANES - 1 - count, 1))
    return jnp.where(lane >= LANES - count, high, pltpu.roll(v, LANES - count, 1))


def spans(sizes, count):
    if sum(sizes) != count:
        sizes = [1] * count
    return [(sum(sizes[:i]), n) for i, n in enumerate(sizes)]


def tiled(v, height):
    rows, cols = v.shape[-2:]
    v = v.reshape(v.shape[:-2] + (rows // height, height, cols // LANES, LANES))
    return jnp.swapaxes(v, -3, -2)


def step_kernel(
    plan, phi_hbm, psi_hbm, tab_hbm, x_hbm, traj_hbm, init_hbm, mob_hbm, dir_ref, stat_ref,
    phi_ref, psi_ref, tab_ref, acc, x_ref, traj_ref, mob_ref, init_ext, mob_ext, wide_init, wide_mob, got, state, temp, gain, cross, start, out, prev,
    z_out, z_got, own_sums, all_sums,
    load_sem, ext_send, ext_recv, in_send, in_recv, row_send, row_recv, back_send, back_recv,
    prev_send, prev_recv, hand_send, hand_recv, edge_send, edge_recv, sum_send, sum_recv, column_in,
):
    K, R, T, Z, CT, H = plan.k, plan.r, plan.t, plan.z, plan.tiles, DEPTH
    rows, cols = plan.rows, plan.cols
    NT = K * T
    G = NT // (2 * SUB)
    keep = 1.0 - damping
    me, z = lax.axis_index("tm"), lax.axis_index("space")
    strip = plan.strip_of(me, z)
    up, down = plan.neighbour(strip, z, -1), plan.neighbour(strip, z, 1)

    barrier = pltpu.get_barrier_semaphore()
    for i in range(1, T):
        pl.semaphore_signal(barrier, inc=1, device_id={"tm": (me + i) % T}, device_id_type=MESH)
    for i in range(1, Z):
        pl.semaphore_signal(barrier, inc=1, device_id={"space": (z + i) % Z}, device_id_type=MESH)
    for other in (up, down):
        pl.semaphore_signal(barrier, inc=1, device_id=other, device_id_type=MESH)

    loads = [
        pltpu.make_async_copy(x_hbm, x_ref, load_sem.at[2]),
        pltpu.make_async_copy(init_hbm, init_ext.at[pl.ds(1, T)], load_sem.at[0]),
        pltpu.make_async_copy(mob_hbm, mob_ext.at[pl.ds(1, T)], load_sem.at[1]),
        pltpu.make_async_copy(tab_hbm, tab_ref, load_sem.at[5]),
        pltpu.make_async_copy(phi_hbm, phi_ref, load_sem.at[6]),
        pltpu.make_async_copy(psi_hbm, psi_ref, load_sem.at[7]),
        pltpu.make_async_copy(mob_hbm, mob_ref, load_sem.at[3]),
        pltpu.make_async_copy(traj_hbm, traj_ref, load_sem.at[4]),
    ]
    for copy in loads:
        copy.start()
    pl.semaphore_wait(barrier, T + Z)
    for i in range(1, T):
        pl.semaphore_signal(column_in, inc=1, device_id={"tm": (me + i) % T}, device_id_type=MESH)

    ins, outs = spans(CHUNKS_IN, CT), spans(CHUNKS_OUT, CT)

    def sent_in(n, i):
        other = (strip + i) % T
        part = pl.ds(*ins[n])
        return pltpu.make_async_remote_copy(
            src_ref=x_ref.at[:, other, part], dst_ref=got.at[pl.ds(me * K, K), part],
            send_sem=in_send.at[n, i], recv_sem=in_recv.at[n, i],
            device_id={"tm": plan.device_of(other, z)}, device_id_type=MESH,
        )

    loads[0].wait()
    for n in range(len(ins)):
        for i in range(1, T):
            sent_in(n, i).start()

    beyond = []
    for n, (src, ext) in enumerate(((init_hbm, init_ext), (mob_hbm, mob_ext))):
        for side in range(2):
            beyond.append(
                pltpu.make_async_remote_copy(
                    src_ref=src.at[0 if side == 0 else T - 1],
                    dst_ref=ext.at[T + 1 if side == 0 else 0],
                    send_sem=ext_send.at[n, side], recv_sem=ext_recv.at[n, 1 - side],
                    device_id={"space": (z + (Z - 1 if side == 0 else 1)) % Z}, device_id_type=MESH,
                )
            )
    for copy in beyond:
        copy.start()

    for copy in loads[1:6]:
        copy.wait()
    got[pl.ds(me * K, K)] = x_ref[:, strip]
    for copy in beyond:
        copy.wait()

    def tile(t):
        return slice(t * LANES, (t + 1) * LANES)

    for i in range(R + 2 * (H - 1)):
        at = R + i - (H - 1)
        for ext, wide in ((init_ext, wide_init), (mob_ext, wide_mob)):
            for t in range(CT):
                line = ext[strip + at // R, t, at % R : at % R + 1, :]
                wide[i, :, t * LANES : (t + 1) * LANES] = jnp.broadcast_to(line, (SUB, LANES))

    def prepare(i, _):
        mobs, bases = [], []
        for t in range(CT):
            u, m = wide_init[i, :, tile(t)], wide_mob[i, :, tile(t)]
            mobs.append(m)
            bases.append(reaction_scale * jnp.maximum(3.0 * u * u - 1.0, 0.0) + 4.0 * m)
        mobs, bases = permuted(mobs), permuted(bases)
        for q in range(G):
            e, o = pl.ds(2 * SUB * q, SUB), pl.ds(2 * SUB * q + SUB, SUB)
            for t in range(CT):
                d_e, d_o, c = tab_ref[q, 0] + bases[t], tab_ref[q, 1] + bases[t], tab_ref[q, 2]
                scale = damping / (d_e * d_o + c * c)
                a_e, a_o, a_c = scale * d_o, scale * d_e, scale * c
                start[i, e, tile(t)] = a_e
                start[i, o, tile(t)] = a_o
                temp[i, pl.ds(SUB * q, SUB), tile(t)] = a_c
                gain[i, e, tile(t)] = a_e * mobs[t]
                gain[i, o, tile(t)] = a_o * mobs[t]
                cross[i, pl.ds(SUB * q, SUB), tile(t)] = a_c * mobs[t]
        return 0

    lax.fori_loop(0, R + 2 * (H - 1), prepare, 0)

    strided = R % SUB == 0

    def lane_tile(j):
        return pl.ds(pl.multiple_of(j * LANES, LANES), LANES)

    def width(tiles):
        return 2 if tiles % 2 == 0 else 1

    for n, (base, tiles) in enumerate(ins):
        for i in range(1, T):
            sent_in(n, i).wait()
        wide = width(tiles)

        def transform(m, _, base=base, wide=wide):
            for r in range(R):
                steps = []
                for w in range(wide):
                    j = base + m * wide + w
                    if strided:
                        flat = got.reshape(NT * CT * R, LANES)
                        steps.append(flat[pl.ds(j * R + r, NT, stride=CT * R), :])
                    else:
                        steps.append(got[:, j, r, :])
                spec = jnp.dot(
                    phi_ref[...], jnp.concatenate(steps, axis=1),
                    precision=HIGHEST, preferred_element_type=jnp.float32,
                )
                for w in range(wide):
                    state[0, r + H, :, lane_tile(base + m * wide + w)] = spec[:, tile(w)]
            return 0

        lax.fori_loop(0, tiles // wide, transform, 0)

    def group(q):
        return pl.ds(pl.multiple_of(q * 2 * SUB, 2 * SUB), 2 * SUB)

    def row_edge(slot, q, side):
        return pltpu.make_async_remote_copy(
            src_ref=state.at[slot, pl.ds(H if side == 0 else R, H), group(q)],
            dst_ref=state.at[slot, pl.ds(R + H if side == 0 else 0, H), group(q)],
            send_sem=row_send.at[slot, q, side], recv_sem=row_recv.at[slot, q, 1 - side],
            device_id=up if side == 0 else down, device_id_type=MESH,
        )

    def parts_of(q):
        at = pl.multiple_of(q * 2 * SUB, 2 * SUB)
        return pl.ds(at, SUB), pl.ds(at + SUB, SUB), pl.ds(pl.multiple_of(q * SUB, SUB), SUB)

    def first(q, _):
        e, o, c = parts_of(q)
        for r in range(R):
            s_e = permuted([state[0, r + H, e, tile(t)] for t in range(CT)])
            s_o = permuted([state[0, r + H, o, tile(t)] for t in range(CT)])
            i = r + H - 1
            for t in range(CT):
                a_e, a_o, a_c = start[i, e, tile(t)], start[i, o, tile(t)], temp[i, c, tile(t)]
                b_e = a_e * s_e[t] - a_c * s_o[t]
                b_o = a_o * s_o[t] + a_c * s_e[t]
                start[i, e, tile(t)] = b_e
                start[i, o, tile(t)] = b_o
                state[0, r + H, e, tile(t)] = b_e
                state[0, r + H, o, tile(t)] = b_o
        for side in range(2):
            row_edge(0, q, side).start()
        return 0

    lax.fori_loop(0, G, first, 0)

    rounds = (SWEEPS - 1) // H
    final_out = start

    def visits(n, final):
        now = n % 2
        later = 1 - now

        def visit(q, _):
            e, o, c_at = parts_of(q)
            for side in range(2):
                row_edge(now, q, side).wait()

            if not final:

                @pl.when(n == 0)
                def _():
                    for r in list(range(1 - H, 0)) + list(range(R, R + H - 1)):
                        start[r + H - 1, group(q), :] = state[0, r + H, group(q), :]

            def from_state(slot):
                return lambda r, part, t: state[slot, r + H, part, tile(t)]

            def from_temp(r, part, t):
                return temp[r + H - 1, part, tile(t)]

            for i in range(1, H + 1):
                source = from_temp if i % 2 == 0 else from_state(now)
                into_temp = i % 2 == 1 and i < H
                slot = later if i == H else now
                for r in range(i - H, R + H - i):
                    y_e = [source(r, e, t) for t in range(CT)]
                    y_o = [source(r, o, t) for t in range(CT)]
                    ends = [(from_left(y[CT - 1], CT), from_right(y[0], CT)) for y in (y_e, y_o)]
                    at = r + H - 1
                    ready = []
                    for t in range(CT):

                        def near(y, end, part):
                            low = y[t - 1] if t else end[0]
                            high = y[t + 1] if t < CT - 1 else end[1]
                            return (source(r - 1, part, t) + source(r + 1, part, t)) + (low + high)

                        n_e, n_o = near(y_e, ends[0], e), near(y_o, ends[1], o)
                        c = cross[at, c_at, tile(t)]
                        new_e = keep * y_e[t] + start[at, e, tile(t)] + (gain[at, e, tile(t)] * n_e - c * n_o)
                        new_o = keep * y_o[t] + start[at, o, tile(t)] + (gain[at, o, tile(t)] * n_o + c * n_e)
                        if final and i == H:
                            ready.append((new_e, new_o))
                        elif into_temp:
                            temp[at, e, tile(t)] = new_e
                            temp[at, o, tile(t)] = new_o
                        else:
                            state[slot, r + H, e, tile(t)] = new_e
                            state[slot, r + H, o, tile(t)] = new_o
                    if ready:
                        for n_part, part in enumerate((e, o)):
                            for t, v in enumerate(permuted([pair[n_part] for pair in ready])):
                                final_out[r, part, tile(t)] = v

            if not final:
                for side in range(2):
                    row_edge(later, q, side).start()

            return 0

        return lax.fori_loop(0, G, visit, 0)

    lax.fori_loop(0, rounds - 1, lambda n, _: visits(n, False), 0)
    visits(rounds - 1, True)

    def sent_back(n, i):
        g = (me + i) % T
        part = pl.ds(*outs[n])
        return pltpu.make_async_remote_copy(
            src_ref=out.at[pl.ds(g * K, K), part], dst_ref=dir_ref.at[:, strip, part],
            send_sem=back_send.at[n, i], recv_sem=back_recv.at[n, i],
            device_id={"tm": g}, device_id_type=MESH,
        )

    def sent_prev(n, i):
        g = (me + i) % T
        part = pl.ds(*outs[n])
        return pltpu.make_async_remote_copy(
            src_ref=out.at[(g * K + NT - 1) % NT, part], dst_ref=prev.at[strip, part],
            send_sem=prev_send.at[n, i], recv_sem=prev_recv.at[n, i],
            device_id={"tm": g}, device_id_type=MESH,
        )

    def hand_on(n):
        part = pl.ds(*outs[n])
        return pltpu.make_async_remote_copy(
            src_ref=dir_ref.at[K - 1, :, part], dst_ref=prev.at[:, part],
            send_sem=hand_send.at[n], recv_sem=hand_recv.at[n],
            device_id={"tm": me + 1 - 2 * (me % 2)}, device_id_type=MESH,
        )

    def z_edge(n, side, g):
        part = pl.ds(*outs[n])
        return pltpu.make_async_remote_copy(
            src_ref=z_out.at[side, part, pl.ds(g * K, K)], dst_ref=z_got.at[1 - side, part],
            send_sem=edge_send.at[n, side, g], recv_sem=edge_recv.at[n, 1 - side],
            device_id={"tm": g, "space": (z + (Z - 1 if side == 0 else 1)) % Z}, device_id_type=MESH,
        )

    pl.semaphore_wait(column_in, T - 1)
    for n, (base, tiles) in enumerate(outs):
        wide = width(tiles)

        def restore(m, _, base=base, wide=wide):
            first = base + m * wide
            for r in range(R):
                steps = jnp.dot(
                    psi_ref[...], final_out[r, :, pl.ds(pl.multiple_of(first * LANES, LANES), wide * LANES)],
                    precision=HIGHEST, preferred_element_type=jnp.float32,
                )
                for w in range(wide):
                    j = first + w
                    if strided:
                        flat = out.reshape(NT * CT * R, LANES)
                        flat[pl.ds(j * R + r, NT, stride=CT * R), :] = steps[:, tile(w)]
                    else:
                        out[:, j, r, :] = steps[:, tile(w)]
                    for side, edge in ((0, 0), (1, R - 1)):
                        if r == edge:
                            z_out[side, j] = steps[:, tile(w)]
            return 0

        lax.fori_loop(0, tiles // wide, restore, 0)
        for side, edge in ((0, 0), (1, T - 1)):

            @pl.when(strip == edge)
            def _():
                for g in range(T):
                    z_edge(n, side, g).start()

        for i in range(1, T):
            sent_back(n, i).start()

            @pl.when((me + i) % T % 2 == 0)
            def _():
                sent_prev(n, i).start()

    even = me % 2 == 0
    dir_ref[:, strip] = out[pl.ds(me * K, K)]

    @pl.when(even)
    def _():
        prev[strip] = out[(me * K + NT - 1) % NT]

    for copy in loads[6:]:
        copy.wait()
    acc[...] = jnp.zeros_like(acc)

    def arrive(j):
        for i in range(1, T):
            sent_back(j, i).wait()

            @pl.when((me + i) % T % 2 == 0)
            def _():
                sent_prev(j, i).wait_send()

        @pl.when(even)
        def _():
            for i in range(1, T):
                sent_prev(j, i).wait_recv()
            hand_on(j).start()

        for side, edge in ((0, 0), (1, T - 1)):

            @pl.when(strip == edge)
            def _():
                for g in range(T):
                    z_edge(j, side, g).wait_send()

            z_edge(j, side, me).wait_recv()

    def handed(j):
        @pl.when(even)
        def _():
            hand_on(j).wait_send()

        @pl.when(me % 2 == 1)
        def _():
            hand_on(j).wait_recv()

    sub = lax.broadcasted_iota(jnp.int32, (R, LANES), 0)
    lane = lax.broadcasted_iota(jnp.int32, (R, LANES), 1)
    has_prev = jnp.minimum(me, 1).astype(jnp.float32)

    def shifted(v, line, side):
        if R == SUB:
            at, by = (0, 1) if side == 0 else (R - 1, R - 1)
            return jnp.where(sub == at, line, pltpu.roll(v, by, 0))
        return jnp.concatenate([line, v[: R - 1]] if side == 0 else [v[1:], line], axis=0)

    def tile_sums(j, k, is_first, t, sums):
        west, east = (j + CT - 1) % CT, (j + 1) % CT
        v = dir_ref[k, t, j]
        above = z_got[0, j, pl.ds(k, 1), :] if t == 0 else dir_ref[k, t - 1, j, R - 1 : R, :]
        below = z_got[1, j, pl.ds(k, 1), :] if t == T - 1 else dir_ref[k, t + 1, j, 0:1, :]
        low = pltpu.roll(jnp.where(lane == LANES - 1, dir_ref[k, t, west], v), 1, 1)
        high = pltpu.roll(jnp.where(lane == 0, dir_ref[k, t, east], v), LANES - 1, 1)
        near = (shifted(v, above, 0) + shifted(v, below, 1)) + (low + high)
        before = prev[t, j] * has_prev if is_first else dir_ref[k - 1, t, j]
        u = traj_ref[k, t, j]
        applied = (v - before) * (1.0 / time_step) + mob_ref[t, j] * (4.0 * v - near)
        applied = applied + (3.0 * reaction_scale * u * u - reaction_scale) * v
        res = x_ref[k, t, j]
        return sums[0] + res * res, sums[1] + res * applied, sums[2] + applied * applied

    def add_sums(j, which):
        def some(k, is_first, sums):
            for t in which:
                sums = tile_sums(j, k, is_first, t, sums)
            return sums

        sums = some(0, True, (acc[0], acc[1], acc[2]))
        sums = lax.fori_loop(1, K, lambda k, a: some(k, False, a), sums)
        for n in range(3):
            acc[n] = sums[n]
        return 0

    def tiles_sums(low, high):
        if high > low:
            lax.fori_loop(low, high, lambda j, _: add_sums(j % CT, range(T)), 0)

    for n, (base, tiles) in enumerate(outs):
        arrive(n)
        if n:
            handed(n - 1)
            tiles_sums(max(outs[n - 1][0], 1), base)
    handed(len(outs) - 1)
    tiles_sums(outs[-1][0], CT + 1)

    at = lax.broadcasted_iota(jnp.int32, (SUB, LANES), 0)
    pack = jnp.zeros((SUB, LANES), jnp.float32)
    for n in range(3):
        pack = jnp.where(at == n, jnp.sum(acc[n], axis=0, keepdims=True), pack)
    own_sums[...] = pack
    index, total_count = me * Z + z, T * Z
    all_sums[index] = pack

    def sent_sum(i):
        other = (index + i) % total_count
        return pltpu.make_async_remote_copy(
            src_ref=own_sums, dst_ref=all_sums.at[index],
            send_sem=sum_send.at[i], recv_sem=sum_recv.at[i],
            device_id={"tm": other // Z, "space": other % Z}, device_id_type=MESH,
        )

    def send_sum(i, _):
        sent_sum(i).start()
        return 0

    def wait_sum(i, _):
        sent_sum(i).wait()
        return 0

    lax.fori_loop(1, total_count, send_sum, 0)
    lax.fori_loop(1, total_count, wait_sum, 0)
    total = all_sums[0]
    for i in range(1, total_count):
        total = total + all_sums[i]
    total = jnp.broadcast_to(jnp.sum(total, axis=1, keepdims=True), (SUB, LANES))
    norm, crossed, squared = total[0:1], total[1:2], total[2:3]
    projection, squared_sum = crossed / norm, squared / norm
    remainder = jnp.maximum(squared_sum - projection * projection, 0.0)
    stat_ref[0:1, :] = crossed / squared
    alpha = jnp.broadcast_to(crossed / squared, (R, LANES))

    def scaled(k, _):
        for t in range(T):
            for j in range(CT):
                dir_ref[k, t, j] = alpha * dir_ref[k, t, j]
        return 0

    lax.fori_loop(0, K, scaled, 0)
    stat_ref[1:2, :] = jnp.sqrt(remainder / squared_sum)


def on_device(trajectory, initial_state, residual, mobility):
    t_count, z_count = lax.axis_size("tm"), lax.axis_size("space")
    steps, rows, cols = residual.shape
    plan = Plan(t_count, z_count, steps, rows, cols)
    count = steps * t_count
    groups = count // (2 * SUB)
    forward, inverse, tables = time_tables(count)
    R, H, tiles = plan.r, DEPTH, plan.tiles
    assert (SWEEPS - 1) % H == 0 and R >= H
    f32 = jnp.float32
    vmem, anywhere = pl.BlockSpec(memory_space=pltpu.VMEM), pl.BlockSpec(memory_space=pl.ANY)
    dma = pltpu.SemaphoreType.DMA
    V = lambda *shape: pltpu.VMEM(shape, f32)
    strips = (steps, t_count, tiles, R, LANES)
    near = R + 2 * (H - 1)
    operands = (
        jnp.asarray(forward), jnp.asarray(inverse), jnp.asarray(tables),
        tiled(residual, R), tiled(trajectory, R), tiled(initial_state, R), tiled(mobility, R),
    )
    direction, stats = pl.pallas_call(
        functools.partial(step_kernel, plan),
        out_shape=[jax.ShapeDtypeStruct(strips, f32), jax.ShapeDtypeStruct((2, LANES), f32)],
        in_specs=[anywhere] * 7,
        out_specs=[vmem, vmem],
        scratch_shapes=[
            V(*forward.shape), V(*inverse.shape), V(*tables.shape), V(3, R, LANES), V(*strips), V(*strips), V(*strips[1:]), V(t_count + 2, *strips[2:]), V(t_count + 2, *strips[2:]),
            V(near, SUB, cols), V(near, SUB, cols),
            V(count, tiles, R, LANES), V(2, R + 2 * H, count, cols), V(near, count, cols),
            V(near, count, cols), V(near, count // 2, cols), V(near, count, cols),
            V(count, tiles, R, LANES), V(*strips[1:]), V(2, tiles, count, LANES), V(2, tiles, steps, LANES),
            V(SUB, LANES), V(t_count * z_count, SUB, LANES),
            dma((8,)), dma((2, 2)), dma((2, 2)), dma((tiles, t_count)), dma((tiles, t_count)),
            dma((2, groups, 2)), dma((2, groups, 2)), dma((tiles, t_count)), dma((tiles, t_count)),
            dma((tiles, t_count)), dma((tiles, t_count)), dma((tiles,)), dma((tiles,)),
            dma((tiles, 2, t_count)), dma((tiles, 2)),
            dma((t_count * z_count,)), dma((t_count * z_count,)), pltpu.SemaphoreType.REGULAR,
        ],
        compiler_params=pltpu.CompilerParams(
            collective_id=0, has_side_effects=True, vmem_limit_bytes=36 * 1024 * 1024
        ),
    )(*[pltpu.with_memory_space_constraint(v, pltpu.HBM) for v in operands])
    update = jnp.swapaxes(direction, -3, -2).reshape(residual.shape)
    return (update, stats[1, 0])


def solution(mesh):
    placed = (P("tm", "space", None), P("space", None), P("tm", "space", None), P("space", None))
    return jax.shard_map(
        on_device,
        mesh=mesh,
        in_specs=placed,
        out_specs=(P("tm", "space", None), P()),
        check_vma=False,
    )
```

```python
import functools
import math
import numpy as np
import jax
import jax.numpy as jnp
from jax import lax
from jax.experimental import pallas as pl
from jax.experimental.pallas import tpu as pltpu
from jax.sharding import PartitionSpec as P

SWEEPS = 16
DEPTH = 3
CHUNKS_IN = [4, 2, 1, 1]
CHUNKS_OUT = [2, 2, 2, 1, 1]
SUB = 8
LANES = 128

circ_weight = 0.2
time_step = 0.01
damping = 0.8
reaction_scale = 40.0

MESH = pl.DeviceIdType.MESH
HIGHEST = lax.Precision.HIGHEST


def time_tables(count):
    f32 = np.float32
    positions = np.arange(count, dtype=f32)
    pair_ids = np.arange(count // 2, dtype=f32)
    phases = f32(2.0 * np.pi) * pair_ids / f32(count)
    angles = phases[:, None] * positions[None, :]
    forward = np.stack([np.cos(angles), -np.sin(angles)], axis=1).reshape(count, count)
    forward[1] = np.cos(f32(np.pi) * positions)
    inverse = forward.T * np.where(np.arange(count) < 2, f32(1.0), f32(2.0)) / f32(count)
    factor = circ_weight ** (1.0 / count)
    shifts = np.repeat((1.0 - factor * np.cos(phases)) / time_step, 2)
    shifts[1] = (1.0 + factor) / time_step
    coupling = factor * np.sin(phases) / time_step
    weights = circ_weight ** (np.arange(count) / count)
    order = np.arange(count).reshape(-1, SUB, 2).transpose(0, 2, 1).reshape(count)
    forward = (forward * weights[None, :])[order]
    inverse = (inverse / weights[:, None])[:, order]
    tiles = np.stack(
        [shifts[0::2].reshape(-1, SUB), shifts[1::2].reshape(-1, SUB), -coupling.reshape(-1, SUB)], axis=1
    )
    tiles = np.broadcast_to(tiles[..., None], tiles.shape + (LANES,))
    return forward.astype(f32), inverse.astype(f32), np.ascontiguousarray(tiles, dtype=f32)


class Plan:
    def __init__(self, t_count, z_count, steps, rows, cols):
        self.t, self.z = t_count, z_count
        self.k, self.rows, self.cols = steps, rows, cols
        self.r = rows // t_count
        self.tiles = cols // LANES
        self.ring = t_count // 2

    def strip_of(self, i, z):
        chip, core = i // 2, i % 2
        half = self.ring // 2
        place = chip + (chip // half) * (self.ring + half - 1 - 2 * chip)
        return ((place + z) % self.ring) * 2 + core

    def device_of(self, strip, z):
        place, core = (strip // 2 + self.ring - z % self.ring) % self.ring, strip % 2
        half = self.ring // 2
        chip = place + (place // half) * (self.ring + half - 1 - 2 * place)
        return chip * 2 + core

    def neighbour(self, strip, z, step):
        total = self.t * self.z
        g = (z * self.t + strip + step + total) % total
        z2, s2 = g // self.t, g % self.t
        return {"tm": self.device_of(s2, z2), "space": z2}


def permuted(tiles):
    lane = lax.broadcasted_iota(jnp.int32, tiles[0].shape, 1)
    tiles, bit = list(tiles), 1
    while bit < len(tiles):
        high = (lane // bit) % 2 == 1
        for i in range(len(tiles)):
            if not i & bit:
                a, b = tiles[i], tiles[i + bit]
                tiles[i] = jnp.where(high, pltpu.roll(b, bit, 1), a)
                tiles[i + bit] = jnp.where(high, b, pltpu.roll(a, LANES - bit, 1))
        bit *= 2
    return tiles


def from_left(v, count):
    lane = lax.broadcasted_iota(jnp.int32, v.shape, 1)
    low = jnp.where(lane == 0, pltpu.roll(v, 1, 1), pltpu.roll(v, (count + 1) % LANES, 1))
    return jnp.where(lane < count, low, pltpu.roll(v, count % LANES, 1))


def from_right(v, count):
    lane = lax.broadcasted_iota(jnp.int32, v.shape, 1)
    high = jnp.where(lane == LANES - 1, pltpu.roll(v, LANES - 1, 1), pltpu.roll(v, LANES - 1 - count, 1))
    return jnp.where(lane >= LANES - count, high, pltpu.roll(v, LANES - count, 1))


def spans(sizes, count):
    if sum(sizes) != count:
        sizes = [1] * count
    return [(sum(sizes[:i]), n) for i, n in enumerate(sizes)]


def tiled(v, height):
    rows, cols = v.shape[-2:]
    v = v.reshape(v.shape[:-2] + (rows // height, height, cols // LANES, LANES))
    return jnp.swapaxes(v, -3, -2)


def step_kernel(
    plan, phi_hbm, psi_hbm, tab_hbm, x_hbm, traj_hbm, init_hbm, mob_hbm, dir_ref, stat_ref,
    phi_ref, psi_ref, tab_ref, acc, x_ref, traj_ref, mob_ref, init_ext, mob_ext, wide_init, wide_mob, got, state, temp, gain, cross, start, out, prev,
    z_out, z_got, own_sums, all_sums,
    load_sem, ext_send, ext_recv, in_send, in_recv, row_send, row_recv, back_send, back_recv,
    prev_send, prev_recv, hand_send, hand_recv, edge_send, edge_recv, sum_send, sum_recv, column_in,
):
    K, R, T, Z, CT, H = plan.k, plan.r, plan.t, plan.z, plan.tiles, DEPTH
    rows, cols = plan.rows, plan.cols
    NT = K * T
    G = NT // (2 * SUB)
    keep = 1.0 - damping
    me, z = lax.axis_index("tm"), lax.axis_index("space")
    strip = plan.strip_of(me, z)
    up, down = plan.neighbour(strip, z, -1), plan.neighbour(strip, z, 1)

    barrier = pltpu.get_barrier_semaphore()
    for i in range(1, T):
        pl.semaphore_signal(barrier, inc=1, device_id={"tm": (me + i) % T}, device_id_type=MESH)
    for i in range(1, Z):
        pl.semaphore_signal(barrier, inc=1, device_id={"space": (z + i) % Z}, device_id_type=MESH)
    for other in (up, down):
        pl.semaphore_signal(barrier, inc=1, device_id=other, device_id_type=MESH)

    loads = [
        pltpu.make_async_copy(x_hbm, x_ref, load_sem.at[2]),
        pltpu.make_async_copy(init_hbm, init_ext.at[pl.ds(1, T)], load_sem.at[0]),
        pltpu.make_async_copy(mob_hbm, mob_ext.at[pl.ds(1, T)], load_sem.at[1]),
        pltpu.make_async_copy(tab_hbm, tab_ref, load_sem.at[5]),
        pltpu.make_async_copy(phi_hbm, phi_ref, load_sem.at[6]),
        pltpu.make_async_copy(psi_hbm, psi_ref, load_sem.at[7]),
        pltpu.make_async_copy(mob_hbm, mob_ref, load_sem.at[3]),
        pltpu.make_async_copy(traj_hbm, traj_ref, load_sem.at[4]),
    ]
    for copy in loads:
        copy.start()
    pl.semaphore_wait(barrier, T + Z)
    for i in range(1, T):
        pl.semaphore_signal(column_in, inc=1, device_id={"tm": (me + i) % T}, device_id_type=MESH)

    ins, outs = spans(CHUNKS_IN, CT), spans(CHUNKS_OUT, CT)

    def sent_in(n, i):
        other = (strip + i) % T
        part = pl.ds(*ins[n])
        return pltpu.make_async_remote_copy(
            src_ref=x_ref.at[:, other, part], dst_ref=got.at[pl.ds(me * K, K), part],
            send_sem=in_send.at[n, i], recv_sem=in_recv.at[n, i],
            device_id={"tm": plan.device_of(other, z)}, device_id_type=MESH,
        )

    loads[0].wait()
    for n in range(len(ins)):
        for i in range(1, T):
            sent_in(n, i).start()

    beyond = []
    for n, (src, ext) in enumerate(((init_hbm, init_ext), (mob_hbm, mob_ext))):
        for side in range(2):
            beyond.append(
                pltpu.make_async_remote_copy(
                    src_ref=src.at[0 if side == 0 else T - 1],
                    dst_ref=ext.at[T + 1 if side == 0 else 0],
                    send_sem=ext_send.at[n, side], recv_sem=ext_recv.at[n, 1 - side],
                    device_id={"space": (z + (Z - 1 if side == 0 else 1)) % Z}, device_id_type=MESH,
                )
            )
    for copy in beyond:
        copy.start()

    for copy in loads[1:6]:
        copy.wait()
    got[pl.ds(me * K, K)] = x_ref[:, strip]
    for copy in beyond:
        copy.wait()

    def tile(t):
        return slice(t * LANES, (t + 1) * LANES)

    for i in range(R + 2 * (H - 1)):
        at = R + i - (H - 1)
        for ext, wide in ((init_ext, wide_init), (mob_ext, wide_mob)):
            for t in range(CT):
                line = ext[strip + at // R, t, at % R : at % R + 1, :]
                wide[i, :, t * LANES : (t + 1) * LANES] = jnp.broadcast_to(line, (SUB, LANES))

    def prepare(i, _):
        mobs, bases = [], []
        for t in range(CT):
            u, m = wide_init[i, :, tile(t)], wide_mob[i, :, tile(t)]
            mobs.append(m)
            bases.append(reaction_scale * jnp.maximum(3.0 * u * u - 1.0, 0.0) + 4.0 * m)
        mobs, bases = permuted(mobs), permuted(bases)
        for q in range(G):
            e, o = pl.ds(2 * SUB * q, SUB), pl.ds(2 * SUB * q + SUB, SUB)
            for t in range(CT):
                d_e, d_o, c = tab_ref[q, 0] + bases[t], tab_ref[q, 1] + bases[t], tab_ref[q, 2]
                scale = damping / (d_e * d_o + c * c)
                a_e, a_o, a_c = scale * d_o, scale * d_e, scale * c
                start[i, e, tile(t)] = a_e
                start[i, o, tile(t)] = a_o
                temp[i, pl.ds(SUB * q, SUB), tile(t)] = a_c
                gain[i, e, tile(t)] = a_e * mobs[t]
                gain[i, o, tile(t)] = a_o * mobs[t]
                cross[i, pl.ds(SUB * q, SUB), tile(t)] = a_c * mobs[t]
        return 0

    lax.fori_loop(0, R + 2 * (H - 1), prepare, 0)

    strided = R % SUB == 0

    def lane_tile(j):
        return pl.ds(pl.multiple_of(j * LANES, LANES), LANES)

    def width(tiles):
        return 2 if tiles % 2 == 0 else 1

    for n, (base, tiles) in enumerate(ins):
        for i in range(1, T):
            sent_in(n, i).wait()
        wide = width(tiles)

        def transform(m, _, base=base, wide=wide):
            for r in range(R):
                steps = []
                for w in range(wide):
                    j = base + m * wide + w
                    if strided:
                        flat = got.reshape(NT * CT * R, LANES)
                        steps.append(flat[pl.ds(j * R + r, NT, stride=CT * R), :])
                    else:
                        steps.append(got[:, j, r, :])
                spec = jnp.dot(
                    phi_ref[...], jnp.concatenate(steps, axis=1),
                    precision=HIGHEST, preferred_element_type=jnp.float32,
                )
                for w in range(wide):
                    state[0, r + H, :, lane_tile(base + m * wide + w)] = spec[:, tile(w)]
            return 0

        lax.fori_loop(0, tiles // wide, transform, 0)

    def group(q):
        return pl.ds(pl.multiple_of(q * 2 * SUB, 2 * SUB), 2 * SUB)

    def row_edge(slot, q, side):
        return pltpu.make_async_remote_copy(
            src_ref=state.at[slot, pl.ds(H if side == 0 else R, H), group(q)],
            dst_ref=state.at[slot, pl.ds(R + H if side == 0 else 0, H), group(q)],
            send_sem=row_send.at[slot, q, side], recv_sem=row_recv.at[slot, q, 1 - side],
            device_id=up if side == 0 else down, device_id_type=MESH,
        )

    def parts_of(q):
        at = pl.multiple_of(q * 2 * SUB, 2 * SUB)
        return pl.ds(at, SUB), pl.ds(at + SUB, SUB), pl.ds(pl.multiple_of(q * SUB, SUB), SUB)

    def first(q, _):
        e, o, c = parts_of(q)
        for r in range(R):
            s_e = permuted([state[0, r + H, e, tile(t)] for t in range(CT)])
            s_o = permuted([state[0, r + H, o, tile(t)] for t in range(CT)])
            i = r + H - 1
            for t in range(CT):
                a_e, a_o, a_c = start[i, e, tile(t)], start[i, o, tile(t)], temp[i, c, tile(t)]
                b_e = a_e * s_e[t] - a_c * s_o[t]
                b_o = a_o * s_o[t] + a_c * s_e[t]
                start[i, e, tile(t)] = b_e
                start[i, o, tile(t)] = b_o
                state[0, r + H, e, tile(t)] = b_e
                state[0, r + H, o, tile(t)] = b_o
        for side in range(2):
            row_edge(0, q, side).start()
        return 0

    lax.fori_loop(0, G, first, 0)

    rounds = (SWEEPS - 1) // H
    final_out = start

    def visits(n, final):
        now = n % 2
        later = 1 - now

        def visit(q, _):
            e, o, c_at = parts_of(q)
            for side in range(2):
                row_edge(now, q, side).wait()

            if not final:

                @pl.when(n == 0)
                def _():
                    for r in list(range(1 - H, 0)) + list(range(R, R + H - 1)):
                        start[r + H - 1, group(q), :] = state[0, r + H, group(q), :]

            def from_state(slot):
                return lambda r, part, t: state[slot, r + H, part, tile(t)]

            def from_temp(r, part, t):
                return temp[r + H - 1, part, tile(t)]

            for i in range(1, H + 1):
                source = from_temp if i % 2 == 0 else from_state(now)
                into_temp = i % 2 == 1 and i < H
                slot = later if i == H else now
                for r in range(i - H, R + H - i):
                    y_e = [source(r, e, t) for t in range(CT)]
                    y_o = [source(r, o, t) for t in range(CT)]
                    ends = [(from_left(y[CT - 1], CT), from_right(y[0], CT)) for y in (y_e, y_o)]
                    at = r + H - 1
                    ready = []
                    for t in range(CT):

                        def near(y, end, part):
                            low = y[t - 1] if t else end[0]
                            high = y[t + 1] if t < CT - 1 else end[1]
                            return (source(r - 1, part, t) + source(r + 1, part, t)) + (low + high)

                        n_e, n_o = near(y_e, ends[0], e), near(y_o, ends[1], o)
                        c = cross[at, c_at, tile(t)]
                        new_e = keep * y_e[t] + start[at, e, tile(t)] + (gain[at, e, tile(t)] * n_e - c * n_o)
                        new_o = keep * y_o[t] + start[at, o, tile(t)] + (gain[at, o, tile(t)] * n_o + c * n_e)
                        if final and i == H:
                            ready.append((new_e, new_o))
                        elif into_temp:
                            temp[at, e, tile(t)] = new_e
                            temp[at, o, tile(t)] = new_o
                        else:
                            state[slot, r + H, e, tile(t)] = new_e
                            state[slot, r + H, o, tile(t)] = new_o
                    if ready:
                        for n_part, part in enumerate((e, o)):
                            for t, v in enumerate(permuted([pair[n_part] for pair in ready])):
                                final_out[r, part, tile(t)] = v

            if not final:
                for side in range(2):
                    row_edge(later, q, side).start()

            return 0

        return lax.fori_loop(0, G, visit, 0)

    lax.fori_loop(0, rounds - 1, lambda n, _: visits(n, False), 0)
    visits(rounds - 1, True)

    def sent_back(n, i):
        g = (me + i) % T
        part = pl.ds(*outs[n])
        return pltpu.make_async_remote_copy(
            src_ref=out.at[pl.ds(g * K, K), part], dst_ref=dir_ref.at[:, strip, part],
            send_sem=back_send.at[n, i], recv_sem=back_recv.at[n, i],
            device_id={"tm": g}, device_id_type=MESH,
        )

    def sent_prev(n, i):
        g = (me + i) % T
        part = pl.ds(*outs[n])
        return pltpu.make_async_remote_copy(
            src_ref=out.at[(g * K + NT - 1) % NT, part], dst_ref=prev.at[strip, part],
            send_sem=prev_send.at[n, i], recv_sem=prev_recv.at[n, i],
            device_id={"tm": g}, device_id_type=MESH,
        )

    def hand_on(n):
        part = pl.ds(*outs[n])
        return pltpu.make_async_remote_copy(
            src_ref=dir_ref.at[K - 1, :, part], dst_ref=prev.at[:, part],
            send_sem=hand_send.at[n], recv_sem=hand_recv.at[n],
            device_id={"tm": me + 1 - 2 * (me % 2)}, device_id_type=MESH,
        )

    def z_edge(n, side, g):
        part = pl.ds(*outs[n])
        return pltpu.make_async_remote_copy(
            src_ref=z_out.at[side, part, pl.ds(g * K, K)], dst_ref=z_got.at[1 - side, part],
            send_sem=edge_send.at[n, side, g], recv_sem=edge_recv.at[n, 1 - side],
            device_id={"tm": g, "space": (z + (Z - 1 if side == 0 else 1)) % Z}, device_id_type=MESH,
        )

    pl.semaphore_wait(column_in, T - 1)
    for n, (base, tiles) in enumerate(outs):
        wide = width(tiles)

        def restore(m, _, base=base, wide=wide):
            first = base + m * wide
            for r in range(R):
                steps = jnp.dot(
                    psi_ref[...], final_out[r, :, pl.ds(pl.multiple_of(first * LANES, LANES), wide * LANES)],
                    precision=HIGHEST, preferred_element_type=jnp.float32,
                )
                for w in range(wide):
                    j = first + w
                    if strided:
                        flat = out.reshape(NT * CT * R, LANES)
                        flat[pl.ds(j * R + r, NT, stride=CT * R), :] = steps[:, tile(w)]
                    else:
                        out[:, j, r, :] = steps[:, tile(w)]
                    for side, edge in ((0, 0), (1, R - 1)):
                        if r == edge:
                            z_out[side, j] = steps[:, tile(w)]
            return 0

        lax.fori_loop(0, tiles // wide, restore, 0)
        for side, edge in ((0, 0), (1, T - 1)):

            @pl.when(strip == edge)
            def _():
                for g in range(T):
                    z_edge(n, side, g).start()

        for i in range(1, T):
            sent_back(n, i).start()

            @pl.when((me + i) % T % 2 == 0)
            def _():
                sent_prev(n, i).start()

    even = me % 2 == 0
    dir_ref[:, strip] = out[pl.ds(me * K, K)]

    @pl.when(even)
    def _():
        prev[strip] = out[(me * K + NT - 1) % NT]

    for copy in loads[6:]:
        copy.wait()
    acc[...] = jnp.zeros_like(acc)

    def arrive(j):
        for i in range(1, T):
            sent_back(j, i).wait()

            @pl.when((me + i) % T % 2 == 0)
            def _():
                sent_prev(j, i).wait_send()

        @pl.when(even)
        def _():
            for i in range(1, T):
                sent_prev(j, i).wait_recv()
            hand_on(j).start()

        for side, edge in ((0, 0), (1, T - 1)):

            @pl.when(strip == edge)
            def _():
                for g in range(T):
                    z_edge(j, side, g).wait_send()

            z_edge(j, side, me).wait_recv()

    def handed(j):
        @pl.when(even)
        def _():
            hand_on(j).wait_send()

        @pl.when(me % 2 == 1)
        def _():
            hand_on(j).wait_recv()

    sub = lax.broadcasted_iota(jnp.int32, (R, LANES), 0)
    lane = lax.broadcasted_iota(jnp.int32, (R, LANES), 1)
    has_prev = jnp.minimum(me, 1).astype(jnp.float32)

    def shifted(v, line, side):
        if R == SUB:
            at, by = (0, 1) if side == 0 else (R - 1, R - 1)
            return jnp.where(sub == at, line, pltpu.roll(v, by, 0))
        return jnp.concatenate([line, v[: R - 1]] if side == 0 else [v[1:], line], axis=0)

    def tile_sums(j, k, is_first, t, sums):
        west, east = (j + CT - 1) % CT, (j + 1) % CT
        v = dir_ref[k, t, j]
        above = z_got[0, j, k : k + 1, :] if t == 0 else dir_ref[k, t - 1, j, R - 1 : R, :]
        below = z_got[1, j, k : k + 1, :] if t == T - 1 else dir_ref[k, t + 1, j, 0:1, :]
        low = pltpu.roll(jnp.where(lane == LANES - 1, dir_ref[k, t, west], v), 1, 1)
        high = pltpu.roll(jnp.where(lane == 0, dir_ref[k, t, east], v), LANES - 1, 1)
        near = (shifted(v, above, 0) + shifted(v, below, 1)) + (low + high)
        before = prev[t, j] * has_prev if is_first else dir_ref[k - 1, t, j]
        u = traj_ref[k, t, j]
        applied = (v - before) * (1.0 / time_step) + mob_ref[t, j] * (4.0 * v - near)
        applied = applied + (3.0 * reaction_scale * u * u - reaction_scale) * v
        res = x_ref[k, t, j]
        return sums[0] + res * res, sums[1] + res * applied, sums[2] + applied * applied

    def add_sums(j, which):
        def some(k, is_first, sums):
            for t in which:
                sums = tile_sums(j, k, is_first, t, sums)
            return sums

        sums = some(0, True, (acc[0], acc[1], acc[2]))
        for k in range(1, K):
            sums = some(k, False, sums)
        for n in range(3):
            acc[n] = sums[n]
        return 0

    def tiles_sums(low, high):
        if high > low:
            lax.fori_loop(low, high, lambda j, _: add_sums(j % CT, range(T)), 0)

    for n, (base, tiles) in enumerate(outs):
        arrive(n)
        if n:
            handed(n - 1)
            tiles_sums(max(outs[n - 1][0], 1), base)
    handed(len(outs) - 1)
    tiles_sums(outs[-1][0], CT + 1)

    at = lax.broadcasted_iota(jnp.int32, (SUB, LANES), 0)
    pack = jnp.zeros((SUB, LANES), jnp.float32)
    for n in range(3):
        pack = jnp.where(at == n, jnp.sum(acc[n], axis=0, keepdims=True), pack)
    own_sums[...] = pack
    index, total_count = me * Z + z, T * Z
    all_sums[index] = pack

    def sent_sum(i):
        other = (index + i) % total_count
        return pltpu.make_async_remote_copy(
            src_ref=own_sums, dst_ref=all_sums.at[index],
            send_sem=sum_send.at[i], recv_sem=sum_recv.at[i],
            device_id={"tm": other // Z, "space": other % Z}, device_id_type=MESH,
        )

    def send_sum(i, _):
        sent_sum(i).start()
        return 0

    def wait_sum(i, _):
        sent_sum(i).wait()
        return 0

    for i in range(1, total_count):
        sent_sum(i).start()
    for i in range(1, total_count):
        sent_sum(i).wait()
    total = all_sums[0]
    for i in range(1, total_count):
        total = total + all_sums[i]
    total = jnp.broadcast_to(jnp.sum(total, axis=1, keepdims=True), (SUB, LANES))
    norm, crossed, squared = total[0:1], total[1:2], total[2:3]
    projection, squared_sum = crossed / norm, squared / norm
    remainder = jnp.maximum(squared_sum - projection * projection, 0.0)
    stat_ref[0:1, :] = crossed / squared
    alpha = jnp.broadcast_to(crossed / squared, (R, LANES))

    def scaled(k, _):
        for t in range(T):
            for j in range(CT):
                dir_ref[k, t, j] = alpha * dir_ref[k, t, j]
        return 0

    lax.fori_loop(0, K, scaled, 0)
    stat_ref[1:2, :] = jnp.sqrt(remainder / squared_sum)


def on_device(trajectory, initial_state, residual, mobility):
    t_count, z_count = lax.axis_size("tm"), lax.axis_size("space")
    steps, rows, cols = residual.shape
    plan = Plan(t_count, z_count, steps, rows, cols)
    count = steps * t_count
    groups = count // (2 * SUB)
    forward, inverse, tables = time_tables(count)
    R, H, tiles = plan.r, DEPTH, plan.tiles
    assert (SWEEPS - 1) % H == 0 and R >= H
    f32 = jnp.float32
    vmem, anywhere = pl.BlockSpec(memory_space=pltpu.VMEM), pl.BlockSpec(memory_space=pl.ANY)
    dma = pltpu.SemaphoreType.DMA
    V = lambda *shape: pltpu.VMEM(shape, f32)
    strips = (steps, t_count, tiles, R, LANES)
    near = R + 2 * (H - 1)
    operands = (
        jnp.asarray(forward), jnp.asarray(inverse), jnp.asarray(tables),
        tiled(residual, R), tiled(trajectory, R), tiled(initial_state, R), tiled(mobility, R),
    )
    direction, stats = pl.pallas_call(
        functools.partial(step_kernel, plan),
        out_shape=[jax.ShapeDtypeStruct(strips, f32), jax.ShapeDtypeStruct((2, LANES), f32)],
        in_specs=[anywhere] * 7,
        out_specs=[vmem, vmem],
        scratch_shapes=[
            V(*forward.shape), V(*inverse.shape), V(*tables.shape), V(3, R, LANES), V(*strips), V(*strips), V(*strips[1:]), V(t_count + 2, *strips[2:]), V(t_count + 2, *strips[2:]),
            V(near, SUB, cols), V(near, SUB, cols),
            V(count, tiles, R, LANES), V(2, R + 2 * H, count, cols), V(near, count, cols),
            V(near, count, cols), V(near, count // 2, cols), V(near, count, cols),
            V(count, tiles, R, LANES), V(*strips[1:]), V(2, tiles, count, LANES), V(2, tiles, steps, LANES),
            V(SUB, LANES), V(t_count * z_count, SUB, LANES),
            dma((8,)), dma((2, 2)), dma((2, 2)), dma((tiles, t_count)), dma((tiles, t_count)),
            dma((2, groups, 2)), dma((2, groups, 2)), dma((tiles, t_count)), dma((tiles, t_count)),
            dma((tiles, t_count)), dma((tiles, t_count)), dma((tiles,)), dma((tiles,)),
            dma((tiles, 2, t_count)), dma((tiles, 2)),
            dma((t_count * z_count,)), dma((t_count * z_count,)), pltpu.SemaphoreType.REGULAR,
        ],
        compiler_params=pltpu.CompilerParams(
            collective_id=0, has_side_effects=True, vmem_limit_bytes=36 * 1024 * 1024
        ),
    )(*[pltpu.with_memory_space_constraint(v, pltpu.HBM) for v in operands])
    update = jnp.swapaxes(direction, -3, -2).reshape(residual.shape)
    return (update, stats[1, 0])


def solution(mesh):
    placed = (P("tm", "space", None), P("space", None), P("tm", "space", None), P("space", None))
    return jax.shard_map(
        on_device,
        mesh=mesh,
        in_specs=placed,
        out_specs=(P("tm", "space", None), P()),
        check_vma=False,
    )
```
